32 devices in a mesh: line: 16 (over z, x, core), view: 2 (over y).
Axes of the slice: x: 2, y: 2, z: 4, core: 2. Of those that a mesh axis runs over, the one named last changes fastest.
Arguments:
- light_field: bfloat16 [16, 8, 8, 1024], P('line', None, 'view'), may hold values from -6 to 6
- query_weight: bfloat16 [2, 64, 128], replicated, may hold values from -0.75 to 0.75
- key_weight: bfloat16 [2, 64, 128], replicated, may hold values from -24 to 24
- value_weight: bfloat16 [2, 64, 128], replicated, may hold values from -0.75 to 0.75
- out_weight: bfloat16 [2, 128, 64], replicated, may hold values from -0.5 to 0.5
- conv_first: bfloat16 [3, 3, 64, 64], replicated, may hold values from -0.25 to 0.25
- conv_second: bfloat16 [3, 3, 64, 64], replicated, may hold values from -0.25 to 0.25
Outputs:
- result: bfloat16 [16, 8, 8, 1024], P('line', None, 'view')
The draws below stay inside these ranges and needn't reach their ends.
All inputs are finite; a program needn't handle non-finite values.
Results may differ from the reference program's by a relative error of at most 0.0069.
Values may be sent and summed in bfloat16 or wider, within the bound.
No kernel may reach another device: no remote copies, remote signals or barrier semaphores. Data moves between devices by JAX's collectives and lax.ppermute only.
A program may use at most 64 MiB of HBM per device.

```python
import math
import jax
import jax.numpy as jnp
from jax import lax

UVIEWS = 8
VVIEWS = 8
CHANNELS = 64
ATTN_WIDTH = 128
COLS = 16
ROWS = 16


def paired_weights(key):
    folded = jax.random.fold_in(key, 11)
    first_key, second_key = jax.random.split(folded)
    deviation = CHANNELS ** (-0.5)
    query_part = jnp.clip(jax.random.normal(first_key, (2, CHANNELS, ATTN_WIDTH), jnp.float32) * deviation, -0.75, 0.75)
    fresh_noise = jnp.clip(jax.random.normal(second_key, (2, CHANNELS, ATTN_WIDTH), jnp.float32) * deviation, -0.75, 0.75)
    key_part = fresh_noise
    return (query_part, jnp.clip(key_part, -24.0, 24.0))


def draw_query_weight(key, part):
    return paired_weights(key)[0].astype(jnp.bfloat16)


def draw_key_weight(key, part):
    return paired_weights(key)[1].astype(jnp.bfloat16)


def shard_levels(key, shape, cuts, low, top_value):
    loudness = 1.0
    for axis_at, blocks in cuts:
        heights = jax.random.uniform(jax.random.fold_in(jax.random.fold_in(key, 6), axis_at), (blocks,), jnp.float32, low / len(cuts), top_value / len(cuts))
        loudness = loudness * jnp.repeat(jnp.exp(heights), shape[axis_at] // blocks).reshape((-1,) + (1,) * (len(shape) - 1 - axis_at))
    return loudness


def centred(key, extent, scale, bound, cuts=(), kind=jnp.bfloat16):
    values = scale * jax.random.normal(key, extent, jnp.float32)
    if cuts:
        values = values * shard_levels(key, extent, cuts, -0.22, 0.18)
    return jnp.clip(values, -bound, bound).astype(kind)


def setup_inputs(seed: int = 0) -> dict:
    splits = jax.random.split(jax.random.key(seed), 8)
    return {
        "light_field": centred(splits[0], (ROWS, UVIEWS, VVIEWS, COLS * CHANNELS), 1.0, 6.0, ((0, 16), (2, 2))),
        "query_weight": draw_query_weight(jax.random.fold_in(splits[7], 71), 0),
        "key_weight": draw_key_weight(jax.random.fold_in(splits[7], 71), 0),
        "value_weight": centred(splits[3], (2, CHANNELS, ATTN_WIDTH), CHANNELS ** -0.5, 0.75),
        "out_weight": centred(splits[4], (2, ATTN_WIDTH, CHANNELS), ATTN_WIDTH ** -0.5, 0.5),
        "conv_first": centred(splits[5], (3, 3, CHANNELS, CHANNELS), (9 * CHANNELS) ** -0.5, 0.25),
        "conv_second": centred(splits[6], (3, 3, CHANNELS, CHANNELS), (9 * CHANNELS) ** -0.5, 0.25),
    }


def layer_norm(tokens):
    values = tokens.astype(jnp.float32)
    centre = values - lax.optimization_barrier(jnp.mean(values, axis=-1, keepdims=True))
    spread = lax.optimization_barrier(jnp.mean(centre * centre, axis=-1, keepdims=True))
    return (centre * lax.rsqrt(spread + 1e-05)).astype(jnp.bfloat16)

def project(inputs, matrix):
    return jnp.dot(inputs, matrix, preferred_element_type=jnp.float32).astype(jnp.bfloat16)

def lines_attend(tokens, query_matrix, key_matrix, value_matrix, out_matrix):
    normed = layer_norm(tokens)
    queries = project(normed, query_matrix)
    keys = project(normed, key_matrix)
    values = project(normed, value_matrix)
    scaling = 1.0 / math.sqrt(queries.shape[-1])

    def per_line(operands):
        query_rows, key_rows, value_rows = operands
        scores = jnp.einsum('qa,ka->qk', query_rows.astype(jnp.float32), key_rows.astype(jnp.float32)) * scaling
        exponent = jnp.exp(scores - lax.optimization_barrier(jnp.max(scores, axis=-1, keepdims=True)))
        weights = (exponent / lax.optimization_barrier(jnp.sum(exponent, axis=-1, keepdims=True))).astype(jnp.bfloat16)
        return jnp.dot(weights, value_rows, preferred_element_type=jnp.float32).astype(jnp.bfloat16)
    mixed = lax.map(per_line, (queries, keys, values))
    summed = tokens.astype(jnp.float32) + jnp.dot(mixed, out_matrix, preferred_element_type=jnp.float32)
    return summed.astype(jnp.bfloat16)

def correlate(images, kernel):
    return lax.conv_general_dilated(images.astype(jnp.float32), kernel.astype(jnp.float32), (1, 1), 'SAME', dimension_numbers=('NHWC', 'HWIO', 'NHWC'), precision=lax.Precision.HIGHEST)

def leaky_relu(values):
    return jnp.where(values >= 0, values, 0.1 * values)

def reference(light_field, query_weight, key_weight, value_weight, out_weight, conv_first, conv_second):
    ray_grid = light_field.reshape(ROWS, UVIEWS, VVIEWS, COLS, CHANNELS)
    horizontal = ray_grid.transpose(0, 2, 1, 3, 4).reshape(ROWS * VVIEWS, UVIEWS * COLS, CHANNELS)
    after_rows = lines_attend(horizontal, query_weight[0], key_weight[0], value_weight[0], out_weight[0])
    after_rows = after_rows.reshape(ROWS, VVIEWS, UVIEWS, COLS, CHANNELS)
    vertical = after_rows.transpose(2, 3, 1, 0, 4).reshape(UVIEWS * COLS, VVIEWS * ROWS, CHANNELS)
    second = lines_attend(vertical, query_weight[1], key_weight[1], value_weight[1], out_weight[1])
    second = second.reshape(UVIEWS, COLS, VVIEWS, ROWS, CHANNELS)
    images = second.transpose(0, 2, 3, 1, 4).reshape(UVIEWS * VVIEWS, ROWS, COLS, CHANNELS)
    hidden = leaky_relu(correlate(images, conv_first)).astype(jnp.bfloat16)
    summed = (images.astype(jnp.float32) + correlate(hidden, conv_second)).astype(jnp.bfloat16)
    summed = summed.reshape(UVIEWS, VVIEWS, ROWS, COLS, CHANNELS).transpose(2, 0, 1, 3, 4)
    return summed.reshape(ROWS, UVIEWS, VVIEWS, COLS * CHANNELS)
```

```python
import functools
import math

import jax
import jax.numpy as jnp
from jax import lax
from jax.experimental import pallas as pl
from jax.experimental.pallas import tpu as pltpu
from jax.sharding import PartitionSpec as P

AXES = ("line", "view")
QUERY_BLOCK = 256
F32 = jnp.float32
BF16 = jnp.bfloat16
HALO = 2


def block_ones(lanes, channels):
    rows = lax.broadcasted_iota(jnp.int32, (lanes, lanes), 0) // channels
    cols = lax.broadcasted_iota(jnp.int32, (lanes, lanes), 1) // channels
    return jnp.where(rows == cols, 1.0 / channels, 0.0).astype(F32)


def packed_norm(tokens, channels):
    ones = block_ones(tokens.shape[-1], channels)
    mean = jnp.dot(tokens.astype(BF16), ones.astype(BF16), preferred_element_type=F32)
    centre = tokens - mean
    spread = jnp.dot(
        centre * centre, ones, precision=lax.Precision.HIGHEST, preferred_element_type=F32
    )
    return (centre * lax.rsqrt(spread + 1e-05)).astype(BF16)


def project_halves(normed, query_matrix, key_matrix, value_matrix):
    joined = jnp.concatenate([query_matrix, key_matrix, value_matrix], axis=1)
    nothing = jnp.zeros_like(joined)
    halves = []
    for parts in ([joined, nothing], [nothing, joined]):
        matrix = jnp.concatenate(parts, axis=0)
        halves.append(jnp.dot(normed, matrix, preferred_element_type=F32).astype(BF16))
    return halves


def attend_rows(queries, keys, values, scaling):
    scores = (
        lax.dot_general(queries, keys, (((1,), (1,)), ((), ())), preferred_element_type=F32)
        * scaling
    )
    exponent = jnp.exp(scores - jnp.max(scores, axis=-1, keepdims=True))
    weights = (exponent / jnp.sum(exponent, axis=-1, keepdims=True)).astype(BF16)
    return jnp.dot(weights, values, preferred_element_type=F32).astype(BF16)


def attend_line(queries, keys, values, scaling, scratch):
    tokens, width = queries.shape
    if tokens <= QUERY_BLOCK:
        return attend_rows(queries, keys, values, scaling)
    scratch[0] = queries
    scratch[1] = keys
    scratch[2] = values

    def block(index, carry):
        rows = pl.ds(pl.multiple_of(index * QUERY_BLOCK, QUERY_BLOCK), QUERY_BLOCK)
        scratch[3, rows, :] = attend_rows(scratch[0, rows, :], scratch[1], scratch[2], scaling)
        return carry

    lax.fori_loop(0, tokens // QUERY_BLOCK, block, 0)
    return scratch[3]


def out_halves(out_matrix):
    nothing = jnp.zeros_like(out_matrix)
    return jnp.concatenate(
        [
            jnp.concatenate([out_matrix, nothing], axis=1),
            jnp.concatenate([nothing, out_matrix], axis=1),
        ],
        axis=0,
    )


def rows_kernel(x_ref, wq_ref, wk_ref, wv_ref, wo_ref, o_ref, held, lines):
    all_u, local_v, packed = x_ref.shape
    channels, width = wq_ref.shape
    lanes = 2 * channels
    pairs = packed // lanes
    per_line = pairs * all_u
    scaling = 1.0 / math.sqrt(width)
    for u in range(all_u):
        rows = x_ref[u].astype(F32)
        for pair in range(pairs):
            held[pl.ds((pair * all_u + u) * local_v, local_v), :] = rows[
                :, pair * lanes : (pair + 1) * lanes
            ]
    tokens = jnp.concatenate(
        [held[pl.ds(v, per_line, stride=local_v), :] for v in range(local_v)], axis=0
    )
    normed = packed_norm(tokens, channels)
    low, high = project_halves(normed, wq_ref[...], wk_ref[...], wv_ref[...])
    out_matrix = out_halves(wo_ref[...])
    for v in range(local_v):
        span = slice(v * per_line, (v + 1) * per_line)
        both = jnp.concatenate([low[span], high[span]], axis=0)
        mixed = attend_line(
            both[:, :width], both[:, width : 2 * width], both[:, 2 * width :], scaling, lines
        )
        mixed = jnp.concatenate([mixed[:per_line], mixed[per_line:]], axis=1)
        summed = tokens[span] + jnp.dot(mixed, out_matrix, preferred_element_type=F32)
        held[pl.ds(v, per_line, stride=local_v), :] = summed
    o_ref[...] = held[...].astype(BF16).reshape(o_ref.shape)


def columns_kernel(
    x_ref, wq_ref, wk_ref, wv_ref, wo_ref, o_ref, held, lines, *, local_v, views
):
    sources, chunk, lanes = x_ref.shape
    channels, width = wq_ref.shape
    count = chunk // local_v
    per_line = sources * local_v
    scaling = 1.0 / math.sqrt(width)
    held[...] = x_ref[...].astype(F32).reshape(held.shape)
    tokens = jnp.concatenate(
        [held[pl.ds(row, sources, stride=chunk), :] for row in range(chunk)], axis=0
    )
    normed = packed_norm(tokens, channels)
    halves = project_halves(normed, wq_ref[...], wk_ref[...], wv_ref[...])
    out_matrix = out_halves(wo_ref[...])
    for line in range(count):
        span = slice(line * per_line, (line + 1) * per_line)
        mixed = [
            attend_line(
                half[span, :width],
                half[span, width : 2 * width],
                half[span, 2 * width :],
                scaling,
                lines,
            )
            for half in halves
        ]
        summed = tokens[span] + jnp.dot(
            jnp.concatenate(mixed, axis=1), out_matrix, preferred_element_type=F32
        )
        for v in range(local_v):
            held[pl.ds(line * local_v + v, sources, stride=chunk), :] = summed[
                v * sources : (v + 1) * sources
            ]
    second = held[...].astype(BF16).reshape(sources, chunk, lanes)
    window = o_ref.shape[1]
    for step in range(window):
        shift = (step - HALO) * views
        edge = abs(shift)
        if edge:
            blank = jnp.zeros((edge, chunk, lanes), BF16)
        if shift < 0:
            o_ref[:edge, step] = blank
            o_ref[edge:, step] = second[: sources - edge]
        elif shift > 0:
            o_ref[sources - edge :, step] = blank
            o_ref[: sources - edge, step] = second[edge:]
        else:
            o_ref[:, step] = second


def pair_weights(kernel):
    nothing = jnp.zeros_like(kernel[0, 0])
    parts = []
    for row in range(3):
        left, middle, right = kernel[row, 0], kernel[row, 1], kernel[row, 2]
        parts += [
            jnp.concatenate([middle, left], axis=1),
            jnp.concatenate([right, middle], axis=1),
            jnp.concatenate([nothing, right], axis=1),
            jnp.concatenate([left, nothing], axis=1),
        ]
    return jnp.concatenate(parts, axis=0)


def beside(rows, per_pair):
    blank = jnp.zeros((per_pair, rows.shape[1]), rows.dtype)
    after = jnp.concatenate([rows[per_pair:], blank], axis=0)
    before = jnp.concatenate([blank, rows[:-per_pair]], axis=0)
    lane = lax.broadcasted_iota(jnp.int32, rows.shape, 1)
    return jnp.where(lane < rows.shape[1] // 2, after, before)


def conv_kernel(x_ref, first_ref, second_ref, o_ref, *, all_rows):
    sources, window, chunk, lanes = x_ref.shape
    all_u, local_v, packed = o_ref.shape
    per_pair = all_u * local_v
    pairs = packed // lanes
    rows = sources * chunk
    images = [x_ref[:, step].reshape(rows, lanes) for step in range(window)]
    wide = [jnp.concatenate([image, beside(image, per_pair)], axis=1) for image in images]
    first = pair_weights(first_ref[...])
    here = lax.axis_index("line")
    hidden = []
    for step in range(3):
        summed = jnp.dot(
            jnp.concatenate(wide[step : step + 3], axis=1), first, preferred_element_type=F32
        )
        active = jnp.where(summed >= 0, summed, 0.1 * summed)
        row = here + (step - 1)
        inside = jnp.logical_and(row >= 0, row < all_rows)
        hidden.append(jnp.where(inside, active, 0.0).astype(BF16))
    wide = [jnp.concatenate([image, beside(image, per_pair)], axis=1) for image in hidden]
    second = pair_weights(second_ref[...])
    summed = images[HALO].astype(F32) + jnp.dot(
        jnp.concatenate(wide, axis=1), second, preferred_element_type=F32
    )
    for pair in range(pairs):
        for u in range(all_u):
            start = pair * per_pair + u * local_v
            o_ref[u, :, pair * lanes : (pair + 1) * lanes] = summed[
                start : start + local_v
            ].astype(BF16)


def local(light_field, query_weight, key_weight, value_weight, out_weight, conv_first, conv_second):
    span_rows, all_u, local_v, packed = light_field.shape
    channels, width = query_weight.shape[1:]
    lanes = 2 * channels
    lines, views = lax.axis_size("line"), lax.axis_size("view")
    devices = lines * views
    packed_lines = packed // lanes * all_u
    if span_rows != 1 or packed_lines % devices:
        raise ValueError("unsupported split")
    chunk = packed_lines // devices * local_v

    weights = [
        (query_weight[i], key_weight[i], value_weight[i], out_weight[i]) for i in range(2)
    ]

    def scratch(rows, tokens):
        kept = tokens if tokens > QUERY_BLOCK else 16
        return [pltpu.VMEM((rows, lanes), F32), pltpu.VMEM((4, kept, width), BF16)]

    rows = packed_lines * local_v
    leaving = pl.pallas_call(
        rows_kernel,
        out_shape=jax.ShapeDtypeStruct((devices, chunk, lanes), BF16),
        scratch_shapes=scratch(rows, 2 * packed_lines),
        name="rows",
    )(light_field[0], *weights[0])
    arrived = lax.all_to_all(leaving, AXES, split_axis=0, concat_axis=0, tiled=True)
    window = 2 * HALO + 1
    framed = pl.pallas_call(
        functools.partial(columns_kernel, local_v=local_v, views=views),
        out_shape=jax.ShapeDtypeStruct((devices, window, chunk, lanes), BF16),
        scratch_shapes=scratch(devices * chunk, devices * local_v),
        name="columns",
    )(arrived, *weights[1])
    returned = lax.all_to_all(framed, AXES, split_axis=0, concat_axis=0, tiled=True)
    result = pl.pallas_call(
        functools.partial(conv_kernel, all_rows=lines * span_rows),
        out_shape=jax.ShapeDtypeStruct((all_u, local_v, packed), BF16),
        name="convs",
    )(returned, conv_first, conv_second)
    return result[None]


def solution(mesh):
    placed = (P("line", None, "view", None), P(), P(), P(), P(), P(), P())
    return jax.shard_map(
        local, mesh=mesh, in_specs=placed, out_specs=P("line", None, "view", None), check_vma=False
    )
```

```python
import functools
import math

import jax
import jax.numpy as jnp
from jax import lax
from jax.experimental import pallas as pl
from jax.experimental.pallas import tpu as pltpu
from jax.sharding import PartitionSpec as P

AXES = ("line", "view")
QUERY_BLOCK = 256
F32 = jnp.float32
BF16 = jnp.bfloat16
HALO = 2
VMEM_BYTES = 16 * 1024 * 1024


def block_ones(lanes, channels):
    rows = lax.broadcasted_iota(jnp.int32, (lanes, lanes), 0) // channels
    cols = lax.broadcasted_iota(jnp.int32, (lanes, lanes), 1) // channels
    return jnp.where(rows == cols, 1.0 / channels, 0.0).astype(F32)


def packed_norm(tokens, channels):
    ones = block_ones(tokens.shape[-1], channels)
    mean = jnp.dot(tokens.astype(BF16), ones.astype(BF16), preferred_element_type=F32)
    centre = tokens - mean
    spread = jnp.dot(
        centre * centre, ones, precision=lax.Precision.HIGHEST, preferred_element_type=F32
    )
    return (centre * lax.rsqrt(spread + 1e-05)).astype(BF16)


def project_halves(normed, query_matrix, key_matrix, value_matrix):
    joined = jnp.concatenate([query_matrix, key_matrix, value_matrix], axis=1)
    nothing = jnp.zeros_like(joined)
    halves = []
    for parts in ([joined, nothing], [nothing, joined]):
        matrix = jnp.concatenate(parts, axis=0)
        halves.append(jnp.dot(normed, matrix, preferred_element_type=F32).astype(BF16))
    return halves


def attend_rows(queries, keys, values, scaling):
    scores = (
        lax.dot_general(queries, keys, (((1,), (1,)), ((), ())), preferred_element_type=F32)
        * scaling
    )
    exponent = jnp.exp(scores - jnp.max(scores, axis=-1, keepdims=True))
    weights = (exponent / jnp.sum(exponent, axis=-1, keepdims=True)).astype(BF16)
    return jnp.dot(weights, values, preferred_element_type=F32).astype(BF16)


def attend_line(queries, keys, values, scaling, scratch):
    tokens, width = queries.shape
    if tokens <= QUERY_BLOCK:
        return attend_rows(queries, keys, values, scaling)
    scratch[0] = queries
    scratch[1] = keys
    scratch[2] = values

    def block(index, carry):
        rows = pl.ds(pl.multiple_of(index * QUERY_BLOCK, QUERY_BLOCK), QUERY_BLOCK)
        scratch[3, rows, :] = attend_rows(scratch[0, rows, :], scratch[1], scratch[2], scaling)
        return carry

    lax.fori_loop(0, tokens // QUERY_BLOCK, block, 0)
    return scratch[3]


def out_halves(flipped):
    nothing = jnp.zeros_like(flipped)
    return jnp.concatenate(
        [
            jnp.concatenate([flipped, nothing], axis=1),
            jnp.concatenate([nothing, flipped], axis=1),
        ],
        axis=0,
    )


def project_out(mixed, out_matrix):
    return lax.dot_general(
        mixed, out_matrix, (((1,), (1,)), ((), ())), preferred_element_type=F32
    )


def rows_kernel(
    x_hbm, wq_hbm, wk_hbm, wv_hbm, wo_hbm, o_ref, held, lines, x_ref, wq_ref, wk_ref, wv_ref,
    wo_ref, arrivals,
):
    copies = [
        pltpu.make_async_copy(source.at[0], target, arrivals.at[index])
        for index, (source, target) in enumerate(
            [
                (x_hbm, x_ref),
                (wq_hbm, wq_ref),
                (wk_hbm, wk_ref),
                (wv_hbm, wv_ref),
                (wo_hbm, wo_ref),
            ]
        )
    ]
    for copy in copies:
        copy.start()
    copies[0].wait()
    all_u, local_v, packed = x_ref.shape
    channels, width = wq_ref.shape
    lanes = 2 * channels
    pairs = packed // lanes
    per_line = pairs * all_u
    scaling = 1.0 / math.sqrt(width)
    for u in range(all_u):
        rows = x_ref[u].astype(F32)
        for pair in range(pairs):
            held[pl.ds((pair * all_u + u) * local_v, local_v), :] = rows[
                :, pair * lanes : (pair + 1) * lanes
            ]
    tokens = jnp.concatenate(
        [held[pl.ds(v, per_line, stride=local_v), :] for v in range(local_v)], axis=0
    )
    normed = packed_norm(tokens, channels)
    for copy in copies[1:]:
        copy.wait()
    low, high = project_halves(normed, wq_ref[...], wk_ref[...], wv_ref[...])
    out_matrix = out_halves(wo_ref[...])
    for v in range(local_v):
        span = slice(v * per_line, (v + 1) * per_line)
        both = jnp.concatenate([low[span], high[span]], axis=0)
        mixed = attend_line(
            both[:, :width], both[:, width : 2 * width], both[:, 2 * width :], scaling, lines
        )
        mixed = jnp.concatenate([mixed[:per_line], mixed[per_line:]], axis=1)
        summed = tokens[span] + project_out(mixed, out_matrix)
        held[pl.ds(v, per_line, stride=local_v), :] = summed
    o_ref[...] = held[...].astype(BF16).reshape(o_ref.shape)


def columns_kernel(
    x_ref, wq_ref, wk_ref, wv_ref, wo_ref, o_ref, held, lines, *, local_v, views
):
    sources, chunk, lanes = x_ref.shape
    channels, width = wq_ref.shape[1:]
    count = chunk // local_v
    per_line = sources * local_v
    scaling = 1.0 / math.sqrt(width)
    held[...] = x_ref[...].astype(F32).reshape(held.shape)
    tokens = jnp.concatenate(
        [held[pl.ds(row, sources, stride=chunk), :] for row in range(chunk)], axis=0
    )
    normed = packed_norm(tokens, channels)
    halves = project_halves(normed, wq_ref[1], wk_ref[1], wv_ref[1])
    out_matrix = out_halves(wo_ref[1])
    for line in range(count):
        span = slice(line * per_line, (line + 1) * per_line)
        mixed = [
            attend_line(
                half[span, :width],
                half[span, width : 2 * width],
                half[span, 2 * width :],
                scaling,
                lines,
            )
            for half in halves
        ]
        summed = tokens[span] + project_out(jnp.concatenate(mixed, axis=1), out_matrix)
        for v in range(local_v):
            held[pl.ds(line * local_v + v, sources, stride=chunk), :] = summed[
                v * sources : (v + 1) * sources
            ]
    second = held[...].astype(BF16).reshape(sources, chunk, lanes)
    window = o_ref.shape[1]
    for step in range(window):
        shift = (step - HALO) * views
        edge = abs(shift)
        if edge:
            blank = jnp.zeros((edge, chunk, lanes), BF16)
        if shift < 0:
            o_ref[:edge, step] = blank
            o_ref[edge:, step] = second[: sources - edge]
        elif shift > 0:
            o_ref[sources - edge :, step] = blank
            o_ref[: sources - edge, step] = second[edge:]
        else:
            o_ref[:, step] = second


def pair_weights(kernel):
    nothing = jnp.zeros_like(kernel[0, 0])
    parts = []
    for row in range(3):
        left, middle, right = kernel[row, 0], kernel[row, 1], kernel[row, 2]
        parts += [
            jnp.concatenate([middle, left], axis=1),
            jnp.concatenate([right, middle], axis=1),
            jnp.concatenate([nothing, right], axis=1),
            jnp.concatenate([left, nothing], axis=1),
        ]
    return jnp.concatenate(parts, axis=0)


def beside(rows, per_pair):
    blank = jnp.zeros((per_pair, rows.shape[1]), rows.dtype)
    after = jnp.concatenate([rows[per_pair:], blank], axis=0)
    before = jnp.concatenate([blank, rows[:-per_pair]], axis=0)
    lane = lax.broadcasted_iota(jnp.int32, rows.shape, 1)
    return jnp.where(lane < rows.shape[1] // 2, after, before)


def conv_kernel(x_ref, first_ref, second_ref, o_ref, *, all_rows):
    sources, window, chunk, lanes = x_ref.shape
    all_u, local_v, packed = o_ref.shape
    per_pair = all_u * local_v
    pairs = packed // lanes
    rows = sources * chunk
    images = [x_ref[:, step].reshape(rows, lanes) for step in range(window)]
    wide = [jnp.concatenate([image, beside(image, per_pair)], axis=1) for image in images]
    first = pair_weights(first_ref[...])
    here = lax.axis_index("line")
    hidden = []
    for step in range(3):
        summed = jnp.dot(
            jnp.concatenate(wide[step : step + 3], axis=1), first, preferred_element_type=F32
        )
        active = jnp.where(summed >= 0, summed, 0.1 * summed)
        row = here + (step - 1)
        inside = jnp.logical_and(row >= 0, row < all_rows)
        hidden.append(jnp.where(inside, active, 0.0).astype(BF16))
    wide = [jnp.concatenate([image, beside(image, per_pair)], axis=1) for image in hidden]
    second = pair_weights(second_ref[...])
    summed = images[HALO].astype(F32) + jnp.dot(
        jnp.concatenate(wide, axis=1), second, preferred_element_type=F32
    )
    for pair in range(pairs):
        for u in range(all_u):
            start = pair * per_pair + u * local_v
            o_ref[u, :, pair * lanes : (pair + 1) * lanes] = summed[
                start : start + local_v
            ].astype(BF16)


def local(light_field, query_weight, key_weight, value_weight, out_weight, conv_first, conv_second):
    span_rows, all_u, local_v, packed = light_field.shape
    channels, width = query_weight.shape[1:]
    lanes = 2 * channels
    lines, views = lax.axis_size("line"), lax.axis_size("view")
    devices = lines * views
    packed_lines = packed // lanes * all_u
    if span_rows != 1 or packed_lines % devices:
        raise ValueError("unsupported split")
    chunk = packed_lines // devices * local_v

    weights = (query_weight, key_weight, value_weight, out_weight.transpose(0, 2, 1))
    params = pltpu.CompilerParams(vmem_limit_bytes=VMEM_BYTES)

    def scratch(rows, tokens):
        kept = tokens if tokens > QUERY_BLOCK else 16
        return [pltpu.VMEM((rows, lanes), F32), pltpu.VMEM((4, kept, width), BF16)]

    rows = packed_lines * local_v
    leaving = pl.pallas_call(
        rows_kernel,
        out_shape=jax.ShapeDtypeStruct((devices, chunk, lanes), BF16),
        in_specs=[pl.BlockSpec(memory_space=pltpu.HBM)] * 5,
        scratch_shapes=scratch(rows, 2 * packed_lines)
        + [
            pltpu.VMEM((all_u, local_v, packed), BF16),
            *[pltpu.VMEM((channels, width), BF16)] * 4,
            pltpu.SemaphoreType.DMA((5,)),
        ],
        compiler_params=params,
        name="rows",
    )(*(pltpu.with_memory_space_constraint(a, pltpu.HBM) for a in (light_field, *weights)))
    arrived = lax.all_to_all(leaving, AXES, split_axis=0, concat_axis=0, tiled=True)
    window = 2 * HALO + 1
    framed = pl.pallas_call(
        functools.partial(columns_kernel, local_v=local_v, views=views),
        out_shape=jax.ShapeDtypeStruct((devices, window, chunk, lanes), BF16),
        scratch_shapes=scratch(devices * chunk, devices * local_v),
        compiler_params=params,
        name="columns",
    )(arrived, *weights)
    returned = lax.all_to_all(framed, AXES, split_axis=0, concat_axis=0, tiled=True)
    result = pl.pallas_call(
        functools.partial(conv_kernel, all_rows=lines * span_rows),
        out_shape=jax.ShapeDtypeStruct((all_u, local_v, packed), BF16),
        compiler_params=params,
        name="convs",
    )(returned, conv_first, conv_second)
    return result[None]


def solution(mesh):
    placed = (P("line", None, "view", None), P(), P(), P(), P(), P(), P())
    return jax.shard_map(
        local, mesh=mesh, in_specs=placed, out_specs=P("line", None, "view", None), check_vma=False
    )
```

```python
import functools
import math

import jax
import jax.numpy as jnp
from jax import lax
from jax.experimental import pallas as pl
from jax.experimental.pallas import tpu as pltpu
from jax.sharding import PartitionSpec as P

AXES = ("line", "view")
QUERY_BLOCK = 256
F32 = jnp.float32
BF16 = jnp.bfloat16
SUBLANES = 8
VMEM_BYTES = 16 * 1024 * 1024


def block_ones(lanes, channels):
    rows = lax.broadcasted_iota(jnp.int32, (lanes, lanes), 0) // channels
    cols = lax.broadcasted_iota(jnp.int32, (lanes, lanes), 1) // channels
    return jnp.where(rows == cols, 1.0 / channels, 0.0).astype(F32)


def packed_norm(tokens, channels):
    ones = block_ones(tokens.shape[-1], channels)
    mean = jnp.dot(tokens.astype(BF16), ones.astype(BF16), preferred_element_type=F32)
    centre = tokens - mean
    spread = jnp.dot(
        centre * centre, ones, precision=lax.Precision.HIGHEST, preferred_element_type=F32
    )
    return (centre * lax.rsqrt(spread + 1e-05)).astype(BF16)


def project_halves(normed, query_matrix, key_matrix, value_matrix):
    joined = jnp.concatenate([query_matrix, key_matrix, value_matrix], axis=1)
    nothing = jnp.zeros_like(joined)
    halves = []
    for parts in ([joined, nothing], [nothing, joined]):
        matrix = jnp.concatenate(parts, axis=0)
        halves.append(jnp.dot(normed, matrix, preferred_element_type=F32).astype(BF16))
    return halves


def attend_rows(queries, keys, values, scaling):
    scores = (
        lax.dot_general(queries, keys, (((1,), (1,)), ((), ())), preferred_element_type=F32)
        * scaling
    )
    exponent = jnp.exp(scores - jnp.max(scores, axis=-1, keepdims=True))
    weights = (exponent / jnp.sum(exponent, axis=-1, keepdims=True)).astype(BF16)
    return jnp.dot(weights, values, preferred_element_type=F32).astype(BF16)


def attend_line(queries, keys, values, scaling, scratch):
    tokens, width = queries.shape
    if tokens <= QUERY_BLOCK:
        return attend_rows(queries, keys, values, scaling)
    scratch[0] = queries
    scratch[1] = keys
    scratch[2] = values

    def block(index, carry):
        rows = pl.ds(pl.multiple_of(index * QUERY_BLOCK, QUERY_BLOCK), QUERY_BLOCK)
        scratch[3, rows, :] = attend_rows(scratch[0, rows, :], scratch[1], scratch[2], scaling)
        return carry

    lax.fori_loop(0, tokens // QUERY_BLOCK, block, 0)
    return scratch[3]


def out_halves(flipped):
    nothing = jnp.zeros_like(flipped)
    return jnp.concatenate(
        [
            jnp.concatenate([flipped, nothing], axis=1),
            jnp.concatenate([nothing, flipped], axis=1),
        ],
        axis=0,
    )


def project_out(mixed, out_matrix):
    return lax.dot_general(
        mixed, out_matrix, (((1,), (1,)), ((), ())), preferred_element_type=F32
    )


def rows_kernel(
    x_hbm,
    wq_hbm,
    wk_hbm,
    wv_hbm,
    wo_hbm,
    o_ref,
    held,
    spread,
    leaving,
    lines,
    x_ref,
    wq_ref,
    wk_ref,
    wv_ref,
    wo_ref,
    arrivals,
):
    pulls = [
        (x_hbm, x_ref),
        (wq_hbm, wq_ref),
        (wk_hbm, wk_ref),
        (wv_hbm, wv_ref),
        (wo_hbm, wo_ref),
    ]
    copies = [
        pltpu.make_async_copy(source.at[0], target, arrivals.at[index])
        for index, (source, target) in enumerate(pulls)
    ]
    for copy in copies:
        copy.start()
    all_u, local_v, packed = x_ref.shape
    channels, width = wq_ref.shape
    lanes = 2 * channels
    pairs = packed // lanes
    per_line = pairs * all_u
    owners, chunk = o_ref.shape[:2]
    window = chunk // local_v
    own = window - 2
    scaling = 1.0 / math.sqrt(width)
    copies[0].wait()
    for u in range(all_u):
        rows = x_ref[u].astype(F32)
        for pair in range(pairs):
            held[pl.ds((u * pairs + pair) * local_v, local_v), :] = rows[
                :, pair * lanes : (pair + 1) * lanes
            ]
    tokens = jnp.concatenate(
        [held[pl.ds(v, per_line, stride=local_v), :] for v in range(local_v)], axis=0
    )
    normed = packed_norm(tokens, channels)
    for copy in copies[1:]:
        copy.wait()
    low, high = project_halves(normed, wq_ref[...], wk_ref[...], wv_ref[...])
    out_matrix = out_halves(wo_ref[...])
    place = lax.broadcasted_iota(jnp.int32, (owners, lanes), 0) % (pairs // own)
    for v in range(local_v):
        span = slice(v * per_line, (v + 1) * per_line)
        both = jnp.concatenate([low[span], high[span]], axis=0)
        mixed = attend_line(
            both[:, :width], both[:, width : 2 * width], both[:, 2 * width :], scaling, lines
        )
        mixed = jnp.concatenate([mixed[:per_line], mixed[per_line:]], axis=1)
        spread[v, pl.ds(SUBLANES, per_line), :] = tokens[span] + project_out(mixed, out_matrix)
        for step in range(window):
            part = spread[v, pl.ds(SUBLANES - 1 + step, owners, stride=own), :]
            if step == 0:
                part = jnp.where(place == 0, 0.0, part)
            if step == window - 1:
                part = jnp.where(place == pairs // own - 1, 0.0, part)
            leaving[pl.ds(v * window + step, owners, stride=chunk), :] = part
    o_ref[...] = leaving[...].astype(BF16).reshape(o_ref.shape)


def pair_weights(kernel):
    nothing = jnp.zeros_like(kernel[0, 0])
    parts = []
    for row in range(3):
        left, middle, right = kernel[row, 0], kernel[row, 1], kernel[row, 2]
        parts += [
            jnp.concatenate([middle, left], axis=1),
            jnp.concatenate([right, middle], axis=1),
            jnp.concatenate([nothing, right], axis=1),
            jnp.concatenate([left, nothing], axis=1),
        ]
    return jnp.concatenate(parts, axis=0)


def neighbourhood(before, image, after, row):
    lane = lax.broadcasted_iota(jnp.int32, image.shape, 1)
    wide = jnp.concatenate(
        [image, jnp.where(lane < image.shape[1] // 2, after, before)], axis=1
    )
    blank = jnp.zeros((row, wide.shape[1]), wide.dtype)
    above = jnp.concatenate([blank, wide[:-row]], axis=0)
    below = jnp.concatenate([wide[row:], blank], axis=0)
    return jnp.concatenate([above, wide, below], axis=1).astype(BF16)


def columns_kernel(
    x_ref,
    wq_ref,
    wk_ref,
    wv_ref,
    wo_ref,
    first_ref,
    second_ref,
    o_ref,
    held,
    leaving,
    lines,
    *,
    local_v,
    views,
    places,
):
    sources, chunk, lanes = x_ref.shape
    channels, width = wq_ref.shape[1:]
    window = chunk // local_v
    own = window - 2
    per_line = sources * local_v
    row = views * local_v
    scaling = 1.0 / math.sqrt(width)
    held[...] = x_ref[...].astype(F32).reshape(held.shape)
    tokens = jnp.concatenate(
        [held[pl.ds(step, per_line, stride=window), :] for step in range(window)], axis=0
    )
    normed = packed_norm(tokens, channels)
    halves = project_halves(normed, wq_ref[1], wk_ref[1], wv_ref[1])
    out_matrix = out_halves(wo_ref[1])
    images = []
    for step in range(window):
        span = slice(step * per_line, (step + 1) * per_line)
        mixed = [
            attend_line(
                half[span, :width],
                half[span, width : 2 * width],
                half[span, 2 * width :],
                scaling,
                lines,
            )
            for half in halves
        ]
        summed = tokens[span] + project_out(jnp.concatenate(mixed, axis=1), out_matrix)
        images.append(summed.astype(BF16).astype(F32))

    blank = jnp.zeros_like(images[0])
    edged = [blank, *images, blank]
    summed = jnp.dot(
        jnp.concatenate(
            [neighbourhood(*edged[step : step + 3], row) for step in range(window)], axis=0
        ),
        pair_weights(first_ref[...]),
        preferred_element_type=F32,
    )
    active = jnp.where(summed >= 0, summed, 0.1 * summed).astype(BF16).astype(F32)
    place = (lax.axis_index("line") * views + lax.axis_index("view")) % places
    hidden = [active[step * per_line : (step + 1) * per_line] for step in range(window)]
    hidden[0] = jnp.where(place > 0, hidden[0], 0.0)
    hidden[-1] = jnp.where(place < places - 1, hidden[-1], 0.0)
    summed = jnp.dot(
        jnp.concatenate(
            [neighbourhood(*hidden[step : step + 3], row) for step in range(own)], axis=0
        ),
        pair_weights(second_ref[...]),
        preferred_element_type=F32,
    )
    for step in range(own):
        leaving[pl.ds(step, per_line, stride=own), :] = (
            images[step + 1] + summed[step * per_line : (step + 1) * per_line]
        )
    o_ref[...] = leaving[...].astype(BF16).reshape(o_ref.shape)


def place_kernel(x_ref, o_ref, held):
    sources, chunk, lanes = x_ref.shape
    all_u, local_v, packed = o_ref.shape
    own = chunk // local_v
    places = sources // all_u
    held[...] = x_ref[...].astype(F32).reshape(held.shape)
    for source in range(sources):
        u, place = source // places, source % places
        for step in range(own):
            start = (place * own + step) * lanes
            o_ref[u, :, start : start + lanes] = held[
                pl.ds(source * chunk + step, local_v, stride=own), :
            ].astype(BF16)


def local(light_field, query_weight, key_weight, value_weight, out_weight, conv_first, conv_second):
    span_rows, all_u, local_v, packed = light_field.shape
    channels, width = query_weight.shape[1:]
    lanes = 2 * channels
    lines, views = lax.axis_size("line"), lax.axis_size("view")
    devices = lines * views
    pairs = packed // lanes
    packed_lines = pairs * all_u
    own = packed_lines // devices
    if span_rows != 1 or packed_lines % devices or pairs % own:
        raise ValueError("unsupported split")
    window = own + 2
    places = pairs // own

    weights = (query_weight, key_weight, value_weight, out_weight.transpose(0, 2, 1))
    params = pltpu.CompilerParams(vmem_limit_bytes=VMEM_BYTES)

    def scratch(tokens):
        kept = tokens if tokens > QUERY_BLOCK else 16
        return pltpu.VMEM((4, kept, width), BF16)

    leaving = pl.pallas_call(
        rows_kernel,
        out_shape=jax.ShapeDtypeStruct((devices, local_v * window, lanes), BF16),
        in_specs=[pl.BlockSpec(memory_space=pltpu.HBM)] * 5,
        scratch_shapes=[
            pltpu.VMEM((packed_lines * local_v, lanes), F32),
            pltpu.VMEM((local_v, packed_lines + 2 * SUBLANES, lanes), F32),
            pltpu.VMEM((devices * local_v * window, lanes), F32),
            scratch(2 * packed_lines),
            pltpu.VMEM((all_u, local_v, packed), BF16),
            *[pltpu.VMEM((channels, width), BF16)] * 4,
            pltpu.SemaphoreType.DMA((5,)),
        ],
        compiler_params=params,
        name="rows",
    )(*(pltpu.with_memory_space_constraint(a, pltpu.HBM) for a in (light_field, *weights)))
    arrived = lax.all_to_all(leaving, AXES, split_axis=0, concat_axis=0, tiled=True)
    finished = pl.pallas_call(
        functools.partial(columns_kernel, local_v=local_v, views=views, places=places),
        out_shape=jax.ShapeDtypeStruct((devices, local_v * own, lanes), BF16),
        scratch_shapes=[
            pltpu.VMEM((devices * local_v * window, lanes), F32),
            pltpu.VMEM((devices * local_v * own, lanes), F32),
            scratch(devices * local_v),
        ],
        compiler_params=params,
        name="columns",
    )(arrived, *weights, conv_first, conv_second)
    returned = lax.all_to_all(finished, AXES, split_axis=0, concat_axis=0, tiled=True)
    result = pl.pallas_call(
        place_kernel,
        out_shape=jax.ShapeDtypeStruct((all_u, local_v, packed), BF16),
        scratch_shapes=[pltpu.VMEM((devices * local_v * own, lanes), F32)],
        compiler_params=params,
        name="place",
    )(returned)
    return result[None]


def solution(mesh):
    placed = (P("line", None, "view", None), P(), P(), P(), P(), P(), P())
    return jax.shard_map(
        local, mesh=mesh, in_specs=placed, out_specs=P("line", None, "view", None), check_vma=False
    )
```

```python
import functools
import math

import jax
import jax.numpy as jnp
from jax import lax
from jax.experimental import pallas as pl
from jax.experimental.pallas import tpu as pltpu
from jax.sharding import PartitionSpec as P

AXES = ("line", "view")
QUERY_BLOCK = 256
F32 = jnp.float32
BF16 = jnp.bfloat16
SUBLANES = 8
VMEM_BYTES = 16 * 1024 * 1024


def block_ones(lanes, channels):
    rows = lax.broadcasted_iota(jnp.int32, (lanes, lanes), 0) // channels
    cols = lax.broadcasted_iota(jnp.int32, (lanes, lanes), 1) // channels
    return jnp.where(rows == cols, 1.0 / channels, 0.0).astype(F32)


def packed_norm(tokens, channels):
    ones = block_ones(tokens.shape[-1], channels)
    mean = jnp.dot(tokens.astype(BF16), ones.astype(BF16), preferred_element_type=F32)
    centre = tokens - mean
    square = centre * centre
    upper = square.astype(BF16)
    lower = (square - upper.astype(F32)).astype(BF16)
    spread = jnp.dot(
        jnp.concatenate([upper, lower], axis=1),
        jnp.concatenate([ones, ones], axis=0).astype(BF16),
        preferred_element_type=F32,
    )
    return (centre * lax.rsqrt(spread + 1e-05)).astype(BF16)


def folded_values(value_matrix, flipped):
    return lax.dot_general(
        value_matrix, flipped, (((1,), (1,)), ((), ())), preferred_element_type=F32
    ).astype(BF16)


def both_halves(*parts):
    lower, upper = [], []
    for first, second in parts:
        lower.append(jnp.zeros_like(second) if first is None else first)
        upper.append(jnp.zeros_like(first) if second is None else second)
    return jnp.concatenate(
        [jnp.concatenate(lower, axis=1), jnp.concatenate(upper, axis=1)], axis=0
    )


def exponents(queries, keys, scaling):
    scores = lax.dot_general(
        queries, keys, (((1,), (1,)), ((), ())), preferred_element_type=F32
    )
    top = jnp.max(scores, axis=-1, keepdims=True)
    return jnp.exp((scores - top) * scaling).astype(BF16)


def weigh(low, high, values):
    rows, lanes = low.shape[0], values.shape[1] // 2
    summed = jnp.dot(
        jnp.concatenate([low, high], axis=0), values, preferred_element_type=F32
    )
    lane = lax.broadcasted_iota(jnp.int32, (rows, 2 * lanes), 1) % lanes
    chosen = jnp.where(lane < lanes // 2, summed[:rows], summed[rows:])
    return chosen[:, :lanes] / chosen[:, lanes:]


def attend_pair(low, high, keys, values, scaling, pieces, mixed):
    count = low.shape[0]
    values = jnp.concatenate([values, jnp.ones_like(values)], axis=1)
    if count <= QUERY_BLOCK:
        if len(keys) == 1:
            both = exponents(jnp.concatenate([low, high], axis=0), keys[0], scaling)
            return weigh(both[:count], both[count:], values)
        return weigh(
            exponents(low, keys[0], scaling), exponents(high, keys[1], scaling), values
        )
    width = low.shape[1]
    key_count = values.shape[0]
    for index, part in enumerate([low, high]):
        pieces[index, :count] = part
    for index, part in enumerate([keys[0], keys[-1], values[:, :width], values[:, width:]]):
        pieces[2 + index, :key_count] = part

    def block(index, carry):
        rows = pl.ds(pl.multiple_of(index * QUERY_BLOCK, QUERY_BLOCK), QUERY_BLOCK)
        mixed[rows, :] = weigh(
            exponents(pieces[0, rows, :], pieces[2, :key_count], scaling),
            exponents(pieces[1, rows, :], pieces[3, :key_count], scaling),
            jnp.concatenate([pieces[4, :key_count], pieces[5, :key_count]], axis=1),
        )
        return carry

    lax.fori_loop(0, count // QUERY_BLOCK, block, 0)
    return mixed[:count]


def rows_kernel(
    x_hbm,
    wq_hbm,
    wk_hbm,
    wv_hbm,
    wo_hbm,
    o_ref,
    held,
    spread,
    leaving,
    lines,
    mixed,
    x_ref,
    wq_ref,
    wk_ref,
    wv_ref,
    wo_ref,
    arrivals,
):
    pulls = [
        (x_hbm, x_ref),
        (wq_hbm, wq_ref),
        (wk_hbm, wk_ref),
        (wv_hbm, wv_ref),
        (wo_hbm, wo_ref),
    ]
    copies = [
        pltpu.make_async_copy(source.at[0], target, arrivals.at[index])
        for index, (source, target) in enumerate(pulls)
    ]
    for copy in copies:
        copy.start()
    all_u, local_v, packed = x_ref.shape
    channels, width = wq_ref.shape
    lanes = 2 * channels
    pairs = packed // lanes
    per_line = pairs * all_u
    owners, chunk = o_ref.shape[:2]
    window = chunk // local_v
    own = window - 2
    scaling = 1.0 / math.sqrt(width)
    copies[0].wait()
    for u in range(all_u):
        rows = x_ref[u].astype(F32)
        for pair in range(pairs):
            held[pl.ds((u * pairs + pair) * local_v, local_v), :] = rows[
                :, pair * lanes : (pair + 1) * lanes
            ]
    tokens = jnp.concatenate(
        [held[pl.ds(v, per_line, stride=local_v), :] for v in range(local_v)], axis=0
    )
    normed = packed_norm(tokens, channels)
    for copy in copies[1:]:
        copy.wait()
    query_matrix, key_matrix = wq_ref[...], wk_ref[...]
    folded = folded_values(wv_ref[...], wo_ref[...])
    projected = jnp.dot(
        normed,
        both_halves(
            (query_matrix, None),
            (key_matrix, None),
            (folded, None),
            (folded, None),
            (None, query_matrix),
            (None, key_matrix),
            (None, folded),
            (None, folded),
        ),
        preferred_element_type=F32,
    ).astype(BF16)
    part = 2 * width + lanes
    place = lax.broadcasted_iota(jnp.int32, (owners, lanes), 0) % (pairs // own)
    for v in range(local_v):
        span = slice(v * per_line, (v + 1) * per_line)
        both = jnp.concatenate([projected[span, :part], projected[span, part:]], axis=0)
        summed = tokens[span] + attend_pair(
            both[:per_line, :width],
            both[per_line:, :width],
            [both[:, width : 2 * width]],
            both[:, 2 * width :],
            scaling,
            lines,
            mixed,
        )
        spread[v, pl.ds(SUBLANES, per_line), :] = summed
        for step in range(window):
            piece = spread[v, pl.ds(SUBLANES - 1 + step, owners, stride=own), :]
            if step == 0:
                piece = jnp.where(place == 0, 0.0, piece)
            if step == window - 1:
                piece = jnp.where(place == pairs // own - 1, 0.0, piece)
            leaving[pl.ds(v * window + step, owners, stride=chunk), :] = piece
    o_ref[...] = leaving[...].astype(BF16).reshape(o_ref.shape)


def pair_weights(kernel):
    nothing = jnp.zeros_like(kernel[0, 0])
    parts = [[], [], [], []]
    for row in range(3):
        left, middle, right = kernel[row, 0], kernel[row, 1], kernel[row, 2]
        parts[0] += [middle, left]
        parts[1] += [right, middle]
        parts[2] += [nothing, right]
        parts[3] += [left, nothing]
    return jnp.concatenate([jnp.concatenate(part, axis=1) for part in parts], axis=0)


def correlate(images, weights, row):
    count, lanes = images[0].shape
    lane = lax.broadcasted_iota(jnp.int32, (count, lanes), 1)
    wide = [
        jnp.concatenate([image, jnp.where(lane < lanes // 2, after, before)], axis=1)
        for before, image, after in zip(images, images[1:], images[2:])
    ]
    terms = jnp.dot(jnp.concatenate(wide, axis=0), weights, preferred_element_type=F32)
    blank = jnp.zeros((row, lanes), F32)
    results = []
    for step in range(len(wide)):
        span = terms[step * count : (step + 1) * count]
        above = jnp.concatenate([blank, span[:-row, :lanes]], axis=0)
        below = jnp.concatenate([span[row:, 2 * lanes :], blank], axis=0)
        results.append(above + span[:, lanes : 2 * lanes] + below)
    return results


def columns_kernel(
    x_ref,
    wq_ref,
    wk_ref,
    wv_ref,
    wo_ref,
    first_ref,
    second_ref,
    o_ref,
    held,
    leaving,
    lines,
    mixed,
    *,
    local_v,
    views,
    places,
):
    sources, chunk, lanes = x_ref.shape
    channels, width = wq_ref.shape[1:]
    window = chunk // local_v
    own = window - 2
    per_line = sources * local_v
    row = views * local_v
    scaling = 1.0 / math.sqrt(width)
    held[...] = x_ref[...].astype(F32).reshape(held.shape)
    tokens = jnp.concatenate(
        [held[pl.ds(step, per_line, stride=window), :] for step in range(window)], axis=0
    )
    normed = packed_norm(tokens, channels)
    query_matrix, key_matrix = wq_ref[1], wk_ref[1]
    folded = folded_values(wv_ref[1], wo_ref[1])
    projected = jnp.dot(
        normed,
        both_halves(
            (query_matrix, None),
            (key_matrix, None),
            (None, query_matrix),
            (None, key_matrix),
            (folded, None),
            (None, folded),
        ),
        preferred_element_type=F32,
    ).astype(BF16)
    images = []
    for step in range(window):
        span = slice(step * per_line, (step + 1) * per_line)
        queries_keys = [projected[span, i * width : (i + 1) * width] for i in range(4)]
        summed = tokens[span] + attend_pair(
            queries_keys[0],
            queries_keys[2],
            queries_keys[1::2],
            projected[span, 4 * width :],
            scaling,
            lines,
            mixed,
        )
        images.append(summed.astype(BF16))

    blank = jnp.zeros_like(images[0])
    hidden = [
        jnp.where(value >= 0, value, 0.1 * value)
        for value in correlate([blank, *images, blank], pair_weights(first_ref[...]), row)
    ]
    place = (lax.axis_index("line") * views + lax.axis_index("view")) % places
    hidden[0] = jnp.where(place > 0, hidden[0], 0.0)
    hidden[-1] = jnp.where(place < places - 1, hidden[-1], 0.0)
    hidden = [value.astype(BF16) for value in hidden]
    for step, value in enumerate(correlate(hidden, pair_weights(second_ref[...]), row)):
        leaving[pl.ds(step, per_line, stride=own), :] = images[step + 1].astype(F32) + value
    o_ref[...] = leaving[...].astype(BF16).reshape(o_ref.shape)


def place_kernel(x_ref, o_ref, held):
    sources, chunk, lanes = x_ref.shape
    all_u, local_v, packed = o_ref.shape
    own = chunk // local_v
    places = sources // all_u
    held[...] = x_ref[...].astype(F32).reshape(held.shape)
    for source in range(sources):
        u, place = source // places, source % places
        for step in range(own):
            start = (place * own + step) * lanes
            o_ref[u, :, start : start + lanes] = held[
                pl.ds(source * chunk + step, local_v, stride=own), :
            ].astype(BF16)


def local(light_field, query_weight, key_weight, value_weight, out_weight, conv_first, conv_second):
    span_rows, all_u, local_v, packed = light_field.shape
    channels, width = query_weight.shape[1:]
    lanes = 2 * channels
    lines, views = lax.axis_size("line"), lax.axis_size("view")
    devices = lines * views
    pairs = packed // lanes
    packed_lines = pairs * all_u
    own = packed_lines // devices
    if span_rows != 1 or packed_lines % devices or pairs % own:
        raise ValueError("unsupported split")
    window = own + 2
    places = pairs // own

    weights = (query_weight, key_weight, value_weight, out_weight.transpose(0, 2, 1))
    params = pltpu.CompilerParams(vmem_limit_bytes=VMEM_BYTES)

    def scratch(tokens):
        kept = tokens if tokens > QUERY_BLOCK else 16
        return [pltpu.VMEM((6, kept, width), BF16), pltpu.VMEM((kept, lanes), F32)]

    leaving = pl.pallas_call(
        rows_kernel,
        out_shape=jax.ShapeDtypeStruct((devices, local_v * window, lanes), BF16),
        in_specs=[pl.BlockSpec(memory_space=pltpu.HBM)] * 5,
        scratch_shapes=[
            pltpu.VMEM((packed_lines * local_v, lanes), F32),
            pltpu.VMEM((local_v, packed_lines + 2 * SUBLANES, lanes), F32),
            pltpu.VMEM((devices * local_v * window, lanes), F32),
            *scratch(2 * packed_lines),
            pltpu.VMEM((all_u, local_v, packed), BF16),
            *[pltpu.VMEM((channels, width), BF16)] * 4,
            pltpu.SemaphoreType.DMA((5,)),
        ],
        compiler_params=params,
        name="rows",
    )(*(pltpu.with_memory_space_constraint(a, pltpu.HBM) for a in (light_field, *weights)))
    arrived = lax.all_to_all(leaving, AXES, split_axis=0, concat_axis=0, tiled=True)
    finished = pl.pallas_call(
        functools.partial(columns_kernel, local_v=local_v, views=views, places=places),
        out_shape=jax.ShapeDtypeStruct((devices, local_v * own, lanes), BF16),
        scratch_shapes=[
            pltpu.VMEM((devices * local_v * window, lanes), F32),
            pltpu.VMEM((devices * local_v * own, lanes), F32),
            *scratch(devices * local_v),
        ],
        compiler_params=params,
        name="columns",
    )(arrived, *weights, conv_first, conv_second)
    returned = lax.all_to_all(finished, AXES, split_axis=0, concat_axis=0, tiled=True)
    result = pl.pallas_call(
        place_kernel,
        out_shape=jax.ShapeDtypeStruct((all_u, local_v, packed), BF16),
        scratch_shapes=[pltpu.VMEM((devices * local_v * own, lanes), F32)],
        compiler_params=params,
        name="place",
    )(returned)
    return result[None]


def solution(mesh):
    placed = (P("line", None, "view", None), P(), P(), P(), P(), P(), P())
    return jax.shard_map(
        local, mesh=mesh, in_specs=placed, out_specs=P("line", None, "view", None), check_vma=False
    )
```

```python
import functools
import math

import jax
import jax.numpy as jnp
from jax import lax
from jax.experimental import pallas as pl
from jax.experimental.pallas import tpu as pltpu
from jax.sharding import PartitionSpec as P

AXES = ("line", "view")
QUERY_BLOCK = 256
F32 = jnp.float32
BF16 = jnp.bfloat16
SUBLANES = 8
VMEM_BYTES = 16 * 1024 * 1024


def block_ones(lanes, channels):
    rows = lax.broadcasted_iota(jnp.int32, (lanes, lanes), 0) // channels
    cols = lax.broadcasted_iota(jnp.int32, (lanes, lanes), 1) // channels
    return jnp.where(rows == cols, 1.0 / channels, 0.0).astype(F32)


def packed_norm(tokens, channels):
    ones = block_ones(tokens.shape[-1], channels)
    mean = jnp.dot(tokens.astype(BF16), ones.astype(BF16), preferred_element_type=F32)
    centre = tokens - mean
    square = centre * centre
    upper = square.astype(BF16)
    lower = (square - upper.astype(F32)).astype(BF16)
    spread = jnp.dot(
        jnp.concatenate([upper, lower], axis=1),
        jnp.concatenate([ones, ones], axis=0).astype(BF16),
        preferred_element_type=F32,
    )
    return (centre * lax.rsqrt(spread + 1e-05)).astype(BF16)


def both_halves(*parts):
    lower, upper = [], []
    for first, second in parts:
        lower.append(jnp.zeros_like(second) if first is None else first)
        upper.append(jnp.zeros_like(first) if second is None else second)
    return jnp.concatenate(
        [jnp.concatenate(lower, axis=1), jnp.concatenate(upper, axis=1)], axis=0
    )


def blend(queries, keys, values, scaling):
    scores = (
        lax.dot_general(keys, queries, (((1,), (1,)), ((), ())), preferred_element_type=F32)
        * scaling
    )
    exponent = jnp.exp(scores - jnp.max(scores, axis=0, keepdims=True))
    weights = exponent * (1.0 / jnp.sum(exponent, axis=0, keepdims=True))
    return jnp.dot(values, weights.astype(BF16), preferred_element_type=F32).astype(BF16)


def in_blocks(count, attend, queries, pieces, mixed):
    if count <= QUERY_BLOCK:
        return attend(*queries)
    for index, part in enumerate(queries):
        pieces[index, :count] = part

    def block(index, carry):
        rows = pl.ds(pl.multiple_of(index * QUERY_BLOCK, QUERY_BLOCK), QUERY_BLOCK)
        mixed[rows, :] = attend(pieces[0, rows, :], pieces[1, rows, :])
        return carry

    lax.fori_loop(0, count // QUERY_BLOCK, block, 0)
    return mixed[:count]


def out_halves(flipped):
    nothing = jnp.zeros_like(flipped)
    return jnp.concatenate(
        [
            jnp.concatenate([flipped, nothing], axis=1),
            jnp.concatenate([nothing, flipped], axis=1),
        ],
        axis=0,
    )


def turned(matrix, normed):
    return lax.dot_general(
        matrix, normed, (((0,), (1,)), ((), ())), preferred_element_type=F32
    ).astype(BF16)


def rows_kernel(
    x_hbm,
    wq_hbm,
    wk_hbm,
    wv_hbm,
    wo_hbm,
    o_ref,
    held,
    spread,
    leaving,
    lines,
    mixed,
    x_ref,
    wq_ref,
    wk_ref,
    wv_ref,
    wo_ref,
    arrivals,
):
    pulls = [
        (x_hbm, x_ref),
        (wq_hbm, wq_ref),
        (wk_hbm, wk_ref),
        (wv_hbm, wv_ref),
        (wo_hbm, wo_ref),
    ]
    copies = [
        pltpu.make_async_copy(source.at[0], target, arrivals.at[index])
        for index, (source, target) in enumerate(pulls)
    ]
    for copy in copies:
        copy.start()
    all_u, local_v, packed = x_ref.shape
    channels, width = wq_ref.shape
    lanes = 2 * channels
    pairs = packed // lanes
    per_line = pairs * all_u
    owners, chunk = o_ref.shape[:2]
    window = chunk // local_v
    own = window - 2
    scaling = 1.0 / math.sqrt(width)
    copies[0].wait()
    for u in range(all_u):
        rows = x_ref[u].astype(F32)
        for pair in range(pairs):
            held[pl.ds((u * pairs + pair) * local_v, local_v), :] = rows[
                :, pair * lanes : (pair + 1) * lanes
            ]
    tokens = jnp.concatenate(
        [held[pl.ds(v, per_line, stride=local_v), :] for v in range(local_v)], axis=0
    )
    normed = packed_norm(tokens, channels)
    for copy in copies[1:]:
        copy.wait()
    swapped = jnp.concatenate([normed[:, channels:], normed[:, :channels]], axis=1)
    every = jnp.concatenate(
        [
            part[v * per_line : (v + 1) * per_line]
            for v in range(local_v)
            for part in (normed, swapped)
        ],
        axis=0,
    )
    nothing = jnp.zeros((channels, width), BF16)
    queries, keys = (
        jnp.dot(
            every, jnp.concatenate([matrix, nothing], axis=0), preferred_element_type=F32
        ).astype(BF16)
        for matrix in (wq_ref[...], wk_ref[...])
    )
    values = turned(jnp.concatenate([wv_ref[...], nothing], axis=0), every)
    out_matrix = jnp.concatenate([wo_ref[...], wo_ref[...]], axis=0)
    lane = lax.broadcasted_iota(jnp.int32, (min(per_line, QUERY_BLOCK), lanes), 1)
    place = lax.broadcasted_iota(jnp.int32, (owners, lanes), 0) % (pairs // own)
    for v in range(local_v):
        span = slice(v * per_line, (v + 1) * per_line)
        line = slice(2 * v * per_line, 2 * (v + 1) * per_line)

        def attend(low, high, line=line):
            blended = blend(
                jnp.concatenate([low, high], axis=0), keys[line], values[:, line], scaling
            )
            terms = jnp.dot(out_matrix, blended, preferred_element_type=F32).T
            return jnp.where(
                lane < channels, terms[: low.shape[0]], terms[low.shape[0] :]
            )

        halves = [queries[line][:per_line], queries[line][per_line:]]
        summed = tokens[span] + in_blocks(per_line, attend, halves, lines, mixed)
        spread[v, pl.ds(SUBLANES, per_line), :] = summed
        for step in range(window):
            piece = spread[v, pl.ds(SUBLANES - 1 + step, owners, stride=own), :]
            if step == 0:
                piece = jnp.where(place == 0, 0.0, piece)
            if step == window - 1:
                piece = jnp.where(place == pairs // own - 1, 0.0, piece)
            leaving[pl.ds(v * window + step, owners, stride=chunk), :] = piece
    o_ref[...] = leaving[...].astype(BF16).reshape(o_ref.shape)


def pair_weights(kernel):
    nothing = jnp.zeros_like(kernel[0, 0])
    parts = [[], [], [], []]
    for row in range(3):
        left, middle, right = kernel[row, 0], kernel[row, 1], kernel[row, 2]
        parts[0] += [middle, left]
        parts[1] += [right, middle]
        parts[2] += [nothing, right]
        parts[3] += [left, nothing]
    return jnp.concatenate([jnp.concatenate(part, axis=1) for part in parts], axis=0)


def correlate(images, weights, row):
    count, lanes = images[0].shape
    lane = lax.broadcasted_iota(jnp.int32, (count, lanes), 1)
    wide = [
        jnp.concatenate([image, jnp.where(lane < lanes // 2, after, before)], axis=1)
        for before, image, after in zip(images, images[1:], images[2:])
    ]
    terms = jnp.dot(jnp.concatenate(wide, axis=0), weights, preferred_element_type=F32)
    blank = jnp.zeros((row, lanes), F32)
    results = []
    for step in range(len(wide)):
        span = terms[step * count : (step + 1) * count]
        above = jnp.concatenate([blank, span[:-row, :lanes]], axis=0)
        below = jnp.concatenate([span[row:, 2 * lanes :], blank], axis=0)
        results.append(above + span[:, lanes : 2 * lanes] + below)
    return results


def columns_kernel(
    x_ref,
    wq_ref,
    wk_ref,
    wv_ref,
    wo_ref,
    first_ref,
    second_ref,
    o_ref,
    held,
    leaving,
    lines,
    mixed,
    *,
    local_v,
    views,
    places,
):
    sources, chunk, lanes = x_ref.shape
    channels, width = wq_ref.shape[1:]
    window = chunk // local_v
    own = window - 2
    per_line = sources * local_v
    row = views * local_v
    scaling = 1.0 / math.sqrt(width)
    held[...] = x_ref[...].astype(F32).reshape(held.shape)
    tokens = jnp.concatenate(
        [held[pl.ds(step, per_line, stride=window), :] for step in range(window)], axis=0
    )
    normed = packed_norm(tokens, channels)
    matrices = [wq_ref[1], wk_ref[1]]
    projected = jnp.dot(
        normed,
        both_halves(*[(m, None) for m in matrices], *[(None, m) for m in matrices]),
        preferred_element_type=F32,
    ).astype(BF16)
    values = turned(both_halves((wv_ref[1], None), (None, wv_ref[1])), normed)
    out_matrix = out_halves(wo_ref[1])
    images = []
    for step in range(window):
        span = slice(step * per_line, (step + 1) * per_line)
        parts = [projected[span, i * width : (i + 1) * width] for i in range(4)]

        def attend(low, high, parts=parts, span=span):
            blended = jnp.concatenate(
                [
                    blend(low, parts[1], values[:width, span], scaling),
                    blend(high, parts[3], values[width:, span], scaling),
                ],
                axis=0,
            )
            return jnp.dot(out_matrix, blended, preferred_element_type=F32).T

        summed = tokens[span] + in_blocks(per_line, attend, parts[::2], lines, mixed)
        images.append(summed.astype(BF16))

    blank = jnp.zeros_like(images[0])
    hidden = [
        jnp.where(value >= 0, value, 0.1 * value)
        for value in correlate([blank, *images, blank], pair_weights(first_ref[...]), row)
    ]
    place = (lax.axis_index("line") * views + lax.axis_index("view")) % places
    hidden[0] = jnp.where(place > 0, hidden[0], 0.0)
    hidden[-1] = jnp.where(place < places - 1, hidden[-1], 0.0)
    hidden = [value.astype(BF16) for value in hidden]
    for step, value in enumerate(correlate(hidden, pair_weights(second_ref[...]), row)):
        leaving[pl.ds(step, per_line, stride=own), :] = images[step + 1].astype(F32) + value
    o_ref[...] = leaving[...].astype(BF16).reshape(o_ref.shape)


def place_kernel(x_ref, o_ref, held):
    sources, chunk, lanes = x_ref.shape
    all_u, local_v, packed = o_ref.shape
    own = chunk // local_v
    places = sources // all_u
    held[...] = x_ref[...].astype(F32).reshape(held.shape)
    for source in range(sources):
        u, place = source // places, source % places
        for step in range(own):
            start = (place * own + step) * lanes
            o_ref[u, :, start : start + lanes] = held[
                pl.ds(source * chunk + step, local_v, stride=own), :
            ].astype(BF16)


def local(light_field, query_weight, key_weight, value_weight, out_weight, conv_first, conv_second):
    span_rows, all_u, local_v, packed = light_field.shape
    channels, width = query_weight.shape[1:]
    lanes = 2 * channels
    lines, views = lax.axis_size("line"), lax.axis_size("view")
    devices = lines * views
    pairs = packed // lanes
    packed_lines = pairs * all_u
    own = packed_lines // devices
    if span_rows != 1 or packed_lines % devices or pairs % own:
        raise ValueError("unsupported split")
    window = own + 2
    places = pairs // own

    weights = (query_weight, key_weight, value_weight, out_weight.transpose(0, 2, 1))
    params = pltpu.CompilerParams(vmem_limit_bytes=VMEM_BYTES)

    def scratch(tokens):
        kept = tokens if tokens > QUERY_BLOCK else 16
        return [pltpu.VMEM((2, kept, width), BF16), pltpu.VMEM((kept, lanes), F32)]

    leaving = pl.pallas_call(
        rows_kernel,
        out_shape=jax.ShapeDtypeStruct((devices, local_v * window, lanes), BF16),
        in_specs=[pl.BlockSpec(memory_space=pltpu.HBM)] * 5,
        scratch_shapes=[
            pltpu.VMEM((packed_lines * local_v, lanes), F32),
            pltpu.VMEM((local_v, packed_lines + 2 * SUBLANES, lanes), F32),
            pltpu.VMEM((devices * local_v * window, lanes), F32),
            *scratch(2 * packed_lines),
            pltpu.VMEM((all_u, local_v, packed), BF16),
            *[pltpu.VMEM((channels, width), BF16)] * 4,
            pltpu.SemaphoreType.DMA((5,)),
        ],
        compiler_params=params,
        name="rows",
    )(*(pltpu.with_memory_space_constraint(a, pltpu.HBM) for a in (light_field, *weights)))
    arrived = lax.all_to_all(leaving, AXES, split_axis=0, concat_axis=0, tiled=True)
    finished = pl.pallas_call(
        functools.partial(columns_kernel, local_v=local_v, views=views, places=places),
        out_shape=jax.ShapeDtypeStruct((devices, local_v * own, lanes), BF16),
        scratch_shapes=[
            pltpu.VMEM((devices * local_v * window, lanes), F32),
            pltpu.VMEM((devices * local_v * own, lanes), F32),
            *scratch(devices * local_v),
        ],
        compiler_params=params,
        name="columns",
    )(arrived, *weights, conv_first, conv_second)
    returned = lax.all_to_all(finished, AXES, split_axis=0, concat_axis=0, tiled=True)
    result = pl.pallas_call(
        place_kernel,
        out_shape=jax.ShapeDtypeStruct((all_u, local_v, packed), BF16),
        scratch_shapes=[pltpu.VMEM((devices * local_v * own, lanes), F32)],
        compiler_params=params,
        name="place",
    )(returned)
    return result[None]


def solution(mesh):
    placed = (P("line", None, "view", None), P(), P(), P(), P(), P(), P())
    return jax.shard_map(
        local, mesh=mesh, in_specs=placed, out_specs=P("line", None, "view", None), check_vma=False
    )
```

```python
import functools
import math

import jax
import jax.numpy as jnp
from jax import lax
from jax.experimental import pallas as pl
from jax.experimental.pallas import tpu as pltpu
from jax.sharding import PartitionSpec as P

AXES = ("line", "view")
QUERY_BLOCK = 256
F32 = jnp.float32
BF16 = jnp.bfloat16
SUBLANES = 8
VMEM_BYTES = 16 * 1024 * 1024


def block_ones(lanes, channels):
    rows = lax.broadcasted_iota(jnp.int32, (lanes, lanes), 0) // channels
    cols = lax.broadcasted_iota(jnp.int32, (lanes, lanes), 1) // channels
    return jnp.where(rows == cols, 1.0 / channels, 0.0).astype(F32)


def packed_norm(tokens, channels):
    ones = block_ones(tokens.shape[-1], channels)
    mean = jnp.dot(tokens.astype(BF16), ones.astype(BF16), preferred_element_type=F32)
    centre = tokens - mean
    square = centre * centre
    upper = square.astype(BF16)
    lower = (square - upper.astype(F32)).astype(BF16)
    spread = jnp.dot(
        jnp.concatenate([upper, lower], axis=1),
        jnp.concatenate([ones, ones], axis=0).astype(BF16),
        preferred_element_type=F32,
    )
    return (centre * lax.rsqrt(spread + 1e-05)).astype(BF16)


def both_halves(*parts):
    lower, upper = [], []
    for first, second in parts:
        lower.append(jnp.zeros_like(second) if first is None else first)
        upper.append(jnp.zeros_like(first) if second is None else second)
    return jnp.concatenate(
        [jnp.concatenate(lower, axis=1), jnp.concatenate(upper, axis=1)], axis=0
    )


def score(queries, keys, scaling):
    return (
        lax.dot_general(keys, queries, (((1,), (1,)), ((), ())), preferred_element_type=F32)
        * scaling
    )


def soften(scores):
    exponent = jnp.exp(scores - jnp.max(scores, axis=0, keepdims=True))
    return (exponent * (1.0 / jnp.sum(exponent, axis=0, keepdims=True))).astype(BF16)


def blend(lines, values, scaling):
    values = values()
    scores = [score(queries, keys, scaling) for queries, keys in lines]
    weights = [soften(part) for part in scores]
    return [
        jnp.dot(part, weight, preferred_element_type=F32).astype(BF16)
        for part, weight in zip(values, weights)
    ]


def in_blocks(count, attend, lines, values, pieces, mixed):
    if count <= QUERY_BLOCK:
        return attend(lines, values)
    values, results = values(), []
    for low, high, keys in lines:
        own_values = values[: len(keys)]
        values = values[len(keys) :]
        for index, part in enumerate([low, high]):
            pieces[index, :count] = part

        def block(index, carry, keys=keys, own_values=own_values):
            rows = pl.ds(pl.multiple_of(index * QUERY_BLOCK, QUERY_BLOCK), QUERY_BLOCK)
            line = (pieces[0, rows, :], pieces[1, rows, :], keys)
            (mixed[rows, :],) = attend([line], lambda: own_values)
            return carry

        lax.fori_loop(0, count // QUERY_BLOCK, block, 0)
        results.append(mixed[:count])
    return results


def out_halves(flipped):
    nothing = jnp.zeros_like(flipped)
    return jnp.concatenate(
        [
            jnp.concatenate([flipped, nothing], axis=1),
            jnp.concatenate([nothing, flipped], axis=1),
        ],
        axis=0,
    )


def project_out(blended, out_matrix):
    return lax.dot_general(
        blended, out_matrix, (((0,), (1,)), ((), ())), preferred_element_type=F32
    )


def turned(matrix, normed):
    return lax.dot_general(
        matrix, normed, (((0,), (1,)), ((), ())), preferred_element_type=F32
    ).astype(BF16)


def rows_kernel(
    x_hbm,
    wq_hbm,
    wk_hbm,
    wv_hbm,
    wo_hbm,
    o_ref,
    held,
    spread,
    leaving,
    lines,
    mixed,
    x_ref,
    wq_ref,
    wk_ref,
    wv_ref,
    wo_ref,
    arrivals,
):
    pulls = [
        (x_hbm, x_ref),
        (wq_hbm, wq_ref),
        (wk_hbm, wk_ref),
        (wv_hbm, wv_ref),
        (wo_hbm, wo_ref),
    ]
    copies = [
        pltpu.make_async_copy(source.at[0], target, arrivals.at[index])
        for index, (source, target) in enumerate(pulls)
    ]
    for copy in copies:
        copy.start()
    all_u, local_v, packed = x_ref.shape
    channels, width = wq_ref.shape
    lanes = 2 * channels
    pairs = packed // lanes
    per_line = pairs * all_u
    owners, chunk = o_ref.shape[:2]
    window = chunk // local_v
    own = window - 2
    scaling = 1.0 / math.sqrt(width)
    for copy in copies:
        copy.wait()
    for u in range(all_u):
        rows = x_ref[u].astype(F32)
        for pair in range(pairs):
            held[pl.ds((u * pairs + pair) * local_v, local_v), :] = rows[
                :, pair * lanes : (pair + 1) * lanes
            ]
    tokens = jnp.concatenate(
        [held[pl.ds(v, per_line, stride=local_v), :] for v in range(local_v)], axis=0
    )
    normed = packed_norm(tokens, channels)
    swapped = jnp.concatenate([normed[:, channels:], normed[:, :channels]], axis=1)
    every = jnp.concatenate(
        [
            part[v * per_line : (v + 1) * per_line]
            for v in range(local_v)
            for part in (normed, swapped)
        ],
        axis=0,
    )
    nothing = jnp.zeros((channels, width), BF16)
    queries, keys = (
        jnp.dot(
            every, jnp.concatenate([matrix, nothing], axis=0), preferred_element_type=F32
        ).astype(BF16)
        for matrix in (wq_ref[...], wk_ref[...])
    )
    out_matrix = jnp.concatenate([wo_ref[...], wo_ref[...]], axis=0)
    lane = lax.broadcasted_iota(jnp.int32, (min(per_line, QUERY_BLOCK), lanes), 1)
    place = lax.broadcasted_iota(jnp.int32, (owners, lanes), 0) % (pairs // own)

    def attend(entries, values):
        blended = blend(
            [(jnp.concatenate([low, high], axis=0), *keys) for low, high, keys in entries],
            values,
            scaling,
        )
        terms = [project_out(part, out_matrix) for part in blended]
        half = lane.shape[0]
        return [jnp.where(lane < channels, term[:half], term[half:]) for term in terms]

    def flipped_values():
        whole = turned(jnp.concatenate([wv_ref[...], nothing], axis=0), every)
        return [whole[:, 2 * v * per_line : 2 * (v + 1) * per_line] for v in range(local_v)]

    entries = []
    for v in range(local_v):
        low = slice(2 * v * per_line, (2 * v + 1) * per_line)
        high = slice((2 * v + 1) * per_line, 2 * (v + 1) * per_line)
        line = slice(2 * v * per_line, 2 * (v + 1) * per_line)
        entries.append((queries[low], queries[high], [keys[line]]))
    results = in_blocks(per_line, attend, entries, flipped_values, lines, mixed)
    for v, terms in enumerate(results):
        span = slice(v * per_line, (v + 1) * per_line)
        spread[v, pl.ds(SUBLANES, per_line), :] = tokens[span] + terms
        for step in range(window):
            piece = spread[v, pl.ds(SUBLANES - 1 + step, owners, stride=own), :]
            if step == 0:
                piece = jnp.where(place == 0, 0.0, piece)
            if step == window - 1:
                piece = jnp.where(place == pairs // own - 1, 0.0, piece)
            leaving[pl.ds(v * window + step, owners, stride=chunk), :] = piece
    o_ref[...] = leaving[...].astype(BF16).reshape(o_ref.shape)


def pair_weights(kernel):
    nothing = jnp.zeros_like(kernel[0, 0])
    parts = [[], [], [], []]
    for row in range(3):
        left, middle, right = kernel[row, 0], kernel[row, 1], kernel[row, 2]
        parts[0] += [middle, left]
        parts[1] += [right, middle]
        parts[2] += [nothing, right]
        parts[3] += [left, nothing]
    return jnp.concatenate([jnp.concatenate(part, axis=1) for part in parts], axis=0)


def correlate(images, weights, row):
    count, lanes = images[0].shape
    lane = lax.broadcasted_iota(jnp.int32, (count, lanes), 1)
    wide = [
        jnp.concatenate([image, jnp.where(lane < lanes // 2, after, before)], axis=1)
        for before, image, after in zip(images, images[1:], images[2:])
    ]
    terms = jnp.dot(jnp.concatenate(wide, axis=0), weights, preferred_element_type=F32)
    blank = jnp.zeros((row, lanes), F32)
    results = []
    for step in range(len(wide)):
        span = terms[step * count : (step + 1) * count]
        above = jnp.concatenate([blank, span[:-row, :lanes]], axis=0)
        below = jnp.concatenate([span[row:, 2 * lanes :], blank], axis=0)
        results.append(above + span[:, lanes : 2 * lanes] + below)
    return results


def columns_kernel(
    x_ref,
    wq_ref,
    wk_ref,
    wv_ref,
    wo_ref,
    first_ref,
    second_ref,
    o_ref,
    held,
    leaving,
    lines,
    mixed,
    *,
    local_v,
    views,
    places,
):
    sources, chunk, lanes = x_ref.shape
    channels, width = wq_ref.shape[1:]
    window = chunk // local_v
    own = window - 2
    per_line = sources * local_v
    row = views * local_v
    scaling = 1.0 / math.sqrt(width)
    held[...] = x_ref[...].astype(F32).reshape(held.shape)
    tokens = jnp.concatenate(
        [held[pl.ds(step, per_line, stride=window), :] for step in range(window)], axis=0
    )
    normed = packed_norm(tokens, channels)
    matrices = [wq_ref[1], wk_ref[1]]
    projected = jnp.dot(
        normed,
        both_halves(*[(m, None) for m in matrices], *[(None, m) for m in matrices]),
        preferred_element_type=F32,
    ).astype(BF16)
    out_matrix = out_halves(wo_ref[1])

    def attend(entries, values):
        blended = blend(
            [
                line
                for low, high, keys in entries
                for line in ((low, keys[0]), (high, keys[1]))
            ],
            values,
            scaling,
        )
        return [
            project_out(jnp.concatenate(pair, axis=0), out_matrix)
            for pair in zip(blended[::2], blended[1::2])
        ]

    spans = [slice(step * per_line, (step + 1) * per_line) for step in range(window)]

    def flipped_values():
        whole = turned(both_halves((wv_ref[1], None), (None, wv_ref[1])), normed)
        return [
            whole[half * width : (half + 1) * width, span] for span in spans for half in range(2)
        ]

    entries = []
    for span in spans:
        parts = [projected[span, i * width : (i + 1) * width] for i in range(4)]
        entries.append((*parts[::2], parts[1::2]))
    results = in_blocks(per_line, attend, entries, flipped_values, lines, mixed)
    images = [(tokens[span] + terms).astype(BF16) for span, terms in zip(spans, results)]

    blank = jnp.zeros_like(images[0])
    hidden = [
        jnp.where(value >= 0, value, 0.1 * value)
        for value in correlate([blank, *images, blank], pair_weights(first_ref[...]), row)
    ]
    place = (lax.axis_index("line") * views + lax.axis_index("view")) % places
    hidden[0] = jnp.where(place > 0, hidden[0], 0.0)
    hidden[-1] = jnp.where(place < places - 1, hidden[-1], 0.0)
    hidden = [value.astype(BF16) for value in hidden]
    for step, value in enumerate(correlate(hidden, pair_weights(second_ref[...]), row)):
        leaving[pl.ds(step, per_line, stride=own), :] = images[step + 1].astype(F32) + value
    o_ref[...] = leaving[...].astype(BF16).reshape(o_ref.shape)


def place_kernel(x_ref, o_ref, held):
    sources, chunk, lanes = x_ref.shape
    all_u, local_v, packed = o_ref.shape
    own = chunk // local_v
    places = sources // all_u
    held[...] = x_ref[...].astype(F32).reshape(held.shape)
    for source in range(sources):
        u, place = source // places, source % places
        for step in range(own):
            start = (place * own + step) * lanes
            o_ref[u, :, start : start + lanes] = held[
                pl.ds(source * chunk + step, local_v, stride=own), :
            ].astype(BF16)


def local(light_field, query_weight, key_weight, value_weight, out_weight, conv_first, conv_second):
    span_rows, all_u, local_v, packed = light_field.shape
    channels, width = query_weight.shape[1:]
    lanes = 2 * channels
    lines, views = lax.axis_size("line"), lax.axis_size("view")
    devices = lines * views
    pairs = packed // lanes
    packed_lines = pairs * all_u
    own = packed_lines // devices
    if span_rows != 1 or packed_lines % devices or pairs % own:
        raise ValueError("unsupported split")
    window = own + 2
    places = pairs // own

    weights = (query_weight, key_weight, value_weight, out_weight.transpose(0, 2, 1))
    params = pltpu.CompilerParams(vmem_limit_bytes=VMEM_BYTES)

    def scratch(tokens):
        kept = tokens if tokens > QUERY_BLOCK else 16
        return [pltpu.VMEM((2, kept, width), BF16), pltpu.VMEM((kept, lanes), F32)]

    leaving = pl.pallas_call(
        rows_kernel,
        out_shape=jax.ShapeDtypeStruct((devices, local_v * window, lanes), BF16),
        in_specs=[pl.BlockSpec(memory_space=pltpu.HBM)] * 5,
        scratch_shapes=[
            pltpu.VMEM((packed_lines * local_v, lanes), F32),
            pltpu.VMEM((local_v, packed_lines + 2 * SUBLANES, lanes), F32),
            pltpu.VMEM((devices * local_v * window, lanes), F32),
            *scratch(2 * packed_lines),
            pltpu.VMEM((all_u, local_v, packed), BF16),
            *[pltpu.VMEM((channels, width), BF16)] * 4,
            pltpu.SemaphoreType.DMA((5,)),
        ],
        compiler_params=params,
        name="rows",
    )(*(pltpu.with_memory_space_constraint(a, pltpu.HBM) for a in (light_field, *weights)))
    arrived = lax.all_to_all(leaving, AXES, split_axis=0, concat_axis=0, tiled=True)
    finished = pl.pallas_call(
        functools.partial(columns_kernel, local_v=local_v, views=views, places=places),
        out_shape=jax.ShapeDtypeStruct((devices, local_v * own, lanes), BF16),
        scratch_shapes=[
            pltpu.VMEM((devices * local_v * window, lanes), F32),
            pltpu.VMEM((devices * local_v * own, lanes), F32),
            *scratch(devices * local_v),
        ],
        compiler_params=params,
        name="columns",
    )(arrived, *weights, conv_first, conv_second)
    returned = lax.all_to_all(finished, AXES, split_axis=0, concat_axis=0, tiled=True)
    result = pl.pallas_call(
        place_kernel,
        out_shape=jax.ShapeDtypeStruct((all_u, local_v, packed), BF16),
        scratch_shapes=[pltpu.VMEM((devices * local_v * own, lanes), F32)],
        compiler_params=params,
        name="place",
    )(returned)
    return result[None]


def solution(mesh):
    placed = (P("line", None, "view", None), P(), P(), P(), P(), P(), P())
    return jax.shard_map(
        local, mesh=mesh, in_specs=placed, out_specs=P("line", None, "view", None), check_vma=False
    )
```

```python
import functools
import math

import jax
import jax.numpy as jnp
from jax import lax
from jax.experimental import pallas as pl
from jax.experimental.pallas import tpu as pltpu
from jax.sharding import PartitionSpec as P

AXES = ("view", "line")
QUERY_BLOCK = 256
F32 = jnp.float32
BF16 = jnp.bfloat16
SUBLANES = 8
VMEM_BYTES = 16 * 1024 * 1024


def block_ones(lanes, channels):
    rows = lax.broadcasted_iota(jnp.int32, (lanes, lanes), 0) // channels
    cols = lax.broadcasted_iota(jnp.int32, (lanes, lanes), 1) // channels
    return jnp.where(rows == cols, 1.0 / channels, 0.0).astype(F32)


def packed_norm(tokens, channels):
    ones = block_ones(tokens.shape[-1], channels)
    mean = jnp.dot(tokens.astype(BF16), ones.astype(BF16), preferred_element_type=F32)
    centre = tokens - mean
    square = centre * centre
    upper = square.astype(BF16)
    lower = (square - upper.astype(F32)).astype(BF16)
    spread = jnp.dot(
        jnp.concatenate([upper, lower], axis=1),
        jnp.concatenate([ones, ones], axis=0).astype(BF16),
        preferred_element_type=F32,
    )
    return (centre * lax.rsqrt(spread + 1e-05)).astype(BF16)


def both_halves(*parts):
    lower, upper = [], []
    for first, second in parts:
        lower.append(jnp.zeros_like(second) if first is None else first)
        upper.append(jnp.zeros_like(first) if second is None else second)
    return jnp.concatenate(
        [jnp.concatenate(lower, axis=1), jnp.concatenate(upper, axis=1)], axis=0
    )


def score(queries, keys, scaling):
    return (
        lax.dot_general(keys, queries, (((1,), (1,)), ((), ())), preferred_element_type=F32)
        * scaling
    )


def soften(scores):
    exponent = jnp.exp(scores - jnp.max(scores, axis=0, keepdims=True))
    return (exponent * (1.0 / jnp.sum(exponent, axis=0, keepdims=True))).astype(BF16)


def blend(lines, values, scaling):
    scores = [score(queries, keys, scaling) for queries, keys in lines]
    values = values()
    weights = [soften(part) for part in scores]
    return [
        jnp.dot(part, weight, preferred_element_type=F32).astype(BF16)
        for part, weight in zip(values, weights)
    ]


def in_blocks(count, attend, lines, values, pieces, mixed):
    if count <= QUERY_BLOCK:
        return attend(lines, values)
    values, results = values(), []
    for low, high, keys in lines:
        own_values = values[: len(keys)]
        values = values[len(keys) :]
        for index, part in enumerate([low, high]):
            pieces[index, :count] = part

        def block(index, carry, keys=keys, own_values=own_values):
            rows = pl.ds(pl.multiple_of(index * QUERY_BLOCK, QUERY_BLOCK), QUERY_BLOCK)
            line = (pieces[0, rows, :], pieces[1, rows, :], keys)
            (mixed[rows, :],) = attend([line], lambda: own_values)
            return carry

        lax.fori_loop(0, count // QUERY_BLOCK, block, 0)
        results.append(mixed[:count])
    return results


def out_halves(flipped):
    nothing = jnp.zeros_like(flipped)
    return jnp.concatenate(
        [
            jnp.concatenate([flipped, nothing], axis=1),
            jnp.concatenate([nothing, flipped], axis=1),
        ],
        axis=0,
    )


def project_out(blended, out_matrix):
    return lax.dot_general(
        blended, out_matrix, (((0,), (1,)), ((), ())), preferred_element_type=F32
    )


def turned(matrix, normed):
    return lax.dot_general(
        matrix, normed, (((0,), (1,)), ((), ())), preferred_element_type=F32
    ).astype(BF16)


def rows_kernel(
    x_hbm,
    wq_hbm,
    wk_hbm,
    wv_hbm,
    wo_hbm,
    o_ref,
    held,
    spread,
    leaving,
    lines,
    mixed,
    x_ref,
    wq_ref,
    wk_ref,
    wv_ref,
    wo_ref,
    arrivals,
):
    pulls = [
        (x_hbm, x_ref),
        (wq_hbm, wq_ref),
        (wk_hbm, wk_ref),
        (wv_hbm, wv_ref),
        (wo_hbm, wo_ref),
    ]
    copies = [
        pltpu.make_async_copy(source.at[0], target, arrivals.at[index])
        for index, (source, target) in enumerate(pulls)
    ]
    for copy in copies:
        copy.start()
    all_u, local_v, packed = x_ref.shape
    channels, width = wq_ref.shape
    lanes = 2 * channels
    pairs = packed // lanes
    per_line = pairs * all_u
    owners, chunk = o_ref.shape[:2]
    window = chunk // local_v
    own = window - 2
    scaling = 1.0 / math.sqrt(width)
    for copy in copies:
        copy.wait()
    for u in range(all_u):
        rows = x_ref[u].astype(F32)
        for pair in range(pairs):
            held[pl.ds((u * pairs + pair) * local_v, local_v), :] = rows[
                :, pair * lanes : (pair + 1) * lanes
            ]
    tokens = jnp.concatenate(
        [held[pl.ds(v, per_line, stride=local_v), :] for v in range(local_v)], axis=0
    )
    normed = packed_norm(tokens, channels)
    matrices = [wq_ref[...], wk_ref[...]]
    projected = jnp.dot(
        normed,
        both_halves(*[(m, None) for m in matrices], *[(None, m) for m in matrices]),
        preferred_element_type=F32,
    ).astype(BF16)
    out_matrix = jnp.concatenate([wo_ref[...], wo_ref[...]], axis=0)
    lane = lax.broadcasted_iota(jnp.int32, (min(per_line, QUERY_BLOCK), lanes), 1)
    place = lax.broadcasted_iota(jnp.int32, (owners, lanes), 0) % (pairs // own)

    def attend(entries, values):
        blended = blend(
            [(jnp.concatenate([low, high], axis=0), *keys) for low, high, keys in entries],
            values,
            scaling,
        )
        terms = [project_out(part, out_matrix) for part in blended]
        half = lane.shape[0]
        return [jnp.where(lane < channels, term[:half], term[half:]) for term in terms]

    def flipped_values():
        swapped = jnp.concatenate([normed[:, channels:], normed[:, :channels]], axis=1)
        every = jnp.concatenate(
            [
                part[v * per_line : (v + 1) * per_line]
                for v in range(local_v)
                for part in (normed, swapped)
            ],
            axis=0,
        )
        padded = jnp.concatenate([wv_ref[...], jnp.zeros_like(wv_ref[...])], axis=0)
        whole = turned(padded, every)
        return [whole[:, 2 * v * per_line : 2 * (v + 1) * per_line] for v in range(local_v)]

    entries = []
    for v in range(local_v):
        span = slice(v * per_line, (v + 1) * per_line)
        parts = [projected[span, i * width : (i + 1) * width] for i in range(4)]
        entries.append((*parts[::2], [jnp.concatenate(parts[1::2], axis=0)]))
    results = in_blocks(per_line, attend, entries, flipped_values, lines, mixed)
    for v, terms in enumerate(results):
        span = slice(v * per_line, (v + 1) * per_line)
        spread[v, pl.ds(SUBLANES, per_line), :] = tokens[span] + terms
        for step in range(window):
            piece = spread[v, pl.ds(SUBLANES - 1 + step, owners, stride=own), :]
            if step == 0:
                piece = jnp.where(place == 0, 0.0, piece)
            if step == window - 1:
                piece = jnp.where(place == pairs // own - 1, 0.0, piece)
            leaving[pl.ds(v * window + step, owners, stride=chunk), :] = piece
    o_ref[...] = leaving[...].astype(BF16).reshape(o_ref.shape)


def pair_weights(kernel):
    nothing = jnp.zeros_like(kernel[0, 0])
    parts = [[], [], [], []]
    for row in range(3):
        left, middle, right = kernel[row, 0], kernel[row, 1], kernel[row, 2]
        parts[0] += [middle, left]
        parts[1] += [right, middle]
        parts[2] += [nothing, right]
        parts[3] += [left, nothing]
    return jnp.concatenate([jnp.concatenate(part, axis=1) for part in parts], axis=0)


def correlate(images, weights, row):
    count, lanes = images[0].shape
    lane = lax.broadcasted_iota(jnp.int32, (count, lanes), 1)
    wide = [
        jnp.concatenate([image, jnp.where(lane < lanes // 2, after, before)], axis=1)
        for before, image, after in zip(images, images[1:], images[2:])
    ]
    terms = jnp.dot(jnp.concatenate(wide, axis=0), weights, preferred_element_type=F32)
    blank = jnp.zeros((row, lanes), F32)
    results = []
    for step in range(len(wide)):
        span = terms[step * count : (step + 1) * count]
        above = jnp.concatenate([blank, span[:-row, :lanes]], axis=0)
        below = jnp.concatenate([span[row:, 2 * lanes :], blank], axis=0)
        results.append(above + span[:, lanes : 2 * lanes] + below)
    return results


def columns_kernel(
    x_ref,
    wq_ref,
    wk_ref,
    wv_ref,
    wo_ref,
    first_ref,
    second_ref,
    o_ref,
    held,
    lines,
    mixed,
    *,
    local_v,
    views,
    places,
):
    sources, chunk, lanes = x_ref.shape
    channels, width = wq_ref.shape[1:]
    window = chunk // local_v
    own = window - 2
    per_line = sources * local_v
    row = views * local_v
    scaling = 1.0 / math.sqrt(width)
    rows = sources // views
    slots = [source % rows * views + source // rows for source in range(sources)]
    for source, slot in enumerate(slots):
        held[pl.ds(slot * chunk, chunk), :] = x_ref[source].astype(F32)
    tokens = jnp.concatenate(
        [held[pl.ds(step, per_line, stride=window), :] for step in range(window)], axis=0
    )
    normed = packed_norm(tokens, channels)
    matrices = [wq_ref[1], wk_ref[1]]
    projected = jnp.dot(
        normed,
        both_halves(*[(m, None) for m in matrices], *[(None, m) for m in matrices]),
        preferred_element_type=F32,
    ).astype(BF16)
    out_matrix = out_halves(wo_ref[1])

    def attend(entries, values):
        blended = blend(
            [
                line
                for low, high, keys in entries
                for line in ((low, keys[0]), (high, keys[1]))
            ],
            values,
            scaling,
        )
        return [
            project_out(jnp.concatenate(pair, axis=0), out_matrix)
            for pair in zip(blended[::2], blended[1::2])
        ]

    spans = [slice(step * per_line, (step + 1) * per_line) for step in range(window)]

    def flipped_values():
        whole = turned(both_halves((wv_ref[1], None), (None, wv_ref[1])), normed)
        return [
            whole[half * width : (half + 1) * width, span] for span in spans for half in range(2)
        ]

    entries = []
    for span in spans:
        parts = [projected[span, i * width : (i + 1) * width] for i in range(4)]
        entries.append((*parts[::2], parts[1::2]))
    results = in_blocks(per_line, attend, entries, flipped_values, lines, mixed)
    images = [(tokens[span] + terms).astype(BF16) for span, terms in zip(spans, results)]

    blank = jnp.zeros_like(images[0])
    hidden = [
        jnp.where(value >= 0, value, 0.1 * value)
        for value in correlate([blank, *images, blank], pair_weights(first_ref[...]), row)
    ]
    place = (lax.axis_index("view") * rows + lax.axis_index("line")) % places
    hidden[0] = jnp.where(place > 0, hidden[0], 0.0)
    hidden[-1] = jnp.where(place < places - 1, hidden[-1], 0.0)
    hidden = [value.astype(BF16) for value in hidden]
    for step, value in enumerate(correlate(hidden, pair_weights(second_ref[...]), row)):
        result = (images[step + 1].astype(F32) + value).astype(BF16)
        for source, slot in enumerate(slots):
            o_ref[source * own + step] = result[slot * local_v : (slot + 1) * local_v]


def local(light_field, query_weight, key_weight, value_weight, out_weight, conv_first, conv_second):
    span_rows, all_u, local_v, packed = light_field.shape
    channels, width = query_weight.shape[1:]
    lanes = 2 * channels
    lines, views = lax.axis_size("line"), lax.axis_size("view")
    devices = lines * views
    pairs = packed // lanes
    packed_lines = pairs * all_u
    own = packed_lines // devices
    if span_rows != 1 or packed_lines % devices or pairs % own:
        raise ValueError("unsupported split")
    window = own + 2
    places = pairs // own

    weights = (query_weight, key_weight, value_weight, out_weight.transpose(0, 2, 1))
    params = pltpu.CompilerParams(vmem_limit_bytes=VMEM_BYTES)

    def scratch(tokens):
        kept = tokens if tokens > QUERY_BLOCK else 16
        return [pltpu.VMEM((2, kept, width), BF16), pltpu.VMEM((kept, lanes), F32)]

    leaving = pl.pallas_call(
        rows_kernel,
        out_shape=jax.ShapeDtypeStruct((devices, local_v * window, lanes), BF16),
        in_specs=[pl.BlockSpec(memory_space=pltpu.HBM)] * 5,
        scratch_shapes=[
            pltpu.VMEM((packed_lines * local_v, lanes), F32),
            pltpu.VMEM((local_v, packed_lines + 2 * SUBLANES, lanes), F32),
            pltpu.VMEM((devices * local_v * window, lanes), F32),
            *scratch(2 * packed_lines),
            pltpu.VMEM((all_u, local_v, packed), BF16),
            *[pltpu.VMEM((channels, width), BF16)] * 4,
            pltpu.SemaphoreType.DMA((5,)),
        ],
        compiler_params=params,
        name="rows",
    )(*(pltpu.with_memory_space_constraint(a, pltpu.HBM) for a in (light_field, *weights)))
    arrived = lax.all_to_all(leaving, AXES, split_axis=0, concat_axis=0, tiled=True)
    finished = pl.pallas_call(
        functools.partial(columns_kernel, local_v=local_v, views=views, places=places),
        out_shape=jax.ShapeDtypeStruct((packed_lines, local_v, lanes), BF16),
        scratch_shapes=[
            pltpu.VMEM((devices * local_v * window, lanes), F32),
            *scratch(devices * local_v),
        ],
        compiler_params=params,
        name="columns",
    )(arrived, *weights, conv_first, conv_second)
    returned = lax.all_to_all(finished, AXES, split_axis=0, concat_axis=0, tiled=True)
    result = returned.reshape(all_u, pairs, local_v, lanes).transpose(0, 2, 1, 3)
    return result.reshape(light_field.shape)


def solution(mesh):
    placed = (P("line", None, "view", None), P(), P(), P(), P(), P(), P())
    return jax.shard_map(
        local, mesh=mesh, in_specs=placed, out_specs=P("line", None, "view", None), check_vma=False
    )
```

```python
import functools
import math

import jax
import jax.numpy as jnp
from jax import lax
from jax.experimental import pallas as pl
from jax.experimental.pallas import tpu as pltpu
from jax.sharding import PartitionSpec as P

AXES = ("view", "line")
QUERY_BLOCK = 256
F32 = jnp.float32
BF16 = jnp.bfloat16
SUBLANES = 8
VMEM_BYTES = 16 * 1024 * 1024


def block_ones(lanes, channels):
    rows = lax.broadcasted_iota(jnp.int32, (lanes, lanes), 0) // channels
    cols = lax.broadcasted_iota(jnp.int32, (lanes, lanes), 1) // channels
    return jnp.where(rows == cols, 1.0 / channels, 0.0).astype(F32)


def packed_norm(tokens, channels):
    ones = block_ones(tokens.shape[-1], channels)
    mean = jnp.dot(tokens.astype(BF16), ones.astype(BF16), preferred_element_type=F32)
    centre = tokens - mean
    square = centre * centre
    upper = square.astype(BF16)
    lower = (square - upper.astype(F32)).astype(BF16)
    spread = jnp.dot(
        jnp.concatenate([upper, lower], axis=1),
        jnp.concatenate([ones, ones], axis=0).astype(BF16),
        preferred_element_type=F32,
    )
    return (centre * lax.rsqrt(spread + 1e-05)).astype(BF16)


def both_halves(*parts):
    lower, upper = [], []
    for first, second in parts:
        lower.append(jnp.zeros_like(second) if first is None else first)
        upper.append(jnp.zeros_like(first) if second is None else second)
    return jnp.concatenate(
        [jnp.concatenate(lower, axis=1), jnp.concatenate(upper, axis=1)], axis=0
    )


def score(queries, keys, scaling):
    return (
        lax.dot_general(keys, queries, (((1,), (1,)), ((), ())), preferred_element_type=F32)
        * scaling
    )


def soften(scores):
    exponent = jnp.exp(scores - jnp.max(scores, axis=0, keepdims=True))
    return (exponent * (1.0 / jnp.sum(exponent, axis=0, keepdims=True))).astype(BF16)


def blend(lines, values, scaling):
    scores = [score(queries, keys, scaling) for queries, keys in lines]
    values = values()
    weights = [soften(part) for part in scores]
    return [
        jnp.dot(part, weight, preferred_element_type=F32).astype(BF16)
        for part, weight in zip(values, weights)
    ]


def in_blocks(count, attend, lines, values, pieces, mixed):
    if count <= QUERY_BLOCK:
        return attend(lines, values)
    values, results = values(), []
    for low, high, keys in lines:
        own_values = values[: len(keys)]
        values = values[len(keys) :]
        for index, part in enumerate([low, high]):
            pieces[index, :count] = part

        def block(index, carry, keys=keys, own_values=own_values):
            rows = pl.ds(pl.multiple_of(index * QUERY_BLOCK, QUERY_BLOCK), QUERY_BLOCK)
            line = (pieces[0, rows, :], pieces[1, rows, :], keys)
            (mixed[rows, :],) = attend([line], lambda: own_values)
            return carry

        lax.fori_loop(0, count // QUERY_BLOCK, block, 0)
        results.append(mixed[:count])
    return results


def out_halves(flipped):
    nothing = jnp.zeros_like(flipped)
    return jnp.concatenate(
        [
            jnp.concatenate([flipped, nothing], axis=1),
            jnp.concatenate([nothing, flipped], axis=1),
        ],
        axis=0,
    )


def project_out(blended, out_matrix):
    return lax.dot_general(
        blended, out_matrix, (((0,), (1,)), ((), ())), preferred_element_type=F32
    )


def turned(matrix, normed):
    return lax.dot_general(
        matrix, normed, (((0,), (1,)), ((), ())), preferred_element_type=F32
    ).astype(BF16)


def rows_kernel(
    x_hbm,
    wq_hbm,
    wk_hbm,
    wv_hbm,
    wo_hbm,
    first_hbm,
    second_hbm,
    o_ref,
    next_wq,
    next_wk,
    next_wv,
    next_wo,
    next_first,
    next_second,
    held,
    spread,
    leaving,
    lines,
    mixed,
    x_ref,
    wq_ref,
    wk_ref,
    wv_ref,
    wo_ref,
    arrivals,
):
    pulls = [
        (x_hbm, x_ref),
        (wq_hbm, wq_ref),
        (wk_hbm, wk_ref),
        (wv_hbm, wv_ref),
        (wo_hbm, wo_ref),
    ]
    copies = [
        pltpu.make_async_copy(source.at[0], target, arrivals.at[index])
        for index, (source, target) in enumerate(pulls)
    ]
    passed_on = [
        (wq_hbm.at[1], next_wq),
        (wk_hbm.at[1], next_wk),
        (wv_hbm.at[1], next_wv),
        (wo_hbm.at[1], next_wo),
        (first_hbm, next_first),
        (second_hbm, next_second),
    ]
    later = [
        pltpu.make_async_copy(source, target, arrivals.at[len(pulls) + index])
        for index, (source, target) in enumerate(passed_on)
    ]
    for copy in copies + later:
        copy.start()
    all_u, local_v, packed = x_ref.shape
    channels, width = wq_ref.shape
    lanes = 2 * channels
    pairs = packed // lanes
    per_line = pairs * all_u
    owners, chunk = o_ref.shape[:2]
    window = chunk // local_v
    own = window - 2
    scaling = 1.0 / math.sqrt(width)
    for copy in copies:
        copy.wait()
    for u in range(all_u):
        rows = x_ref[u].astype(F32)
        for pair in range(pairs):
            held[pl.ds((u * pairs + pair) * local_v, local_v), :] = rows[
                :, pair * lanes : (pair + 1) * lanes
            ]
    tokens = jnp.concatenate(
        [held[pl.ds(v, per_line, stride=local_v), :] for v in range(local_v)], axis=0
    )
    normed = packed_norm(tokens, channels)
    matrices = [wq_ref[...], wk_ref[...]]
    projected = jnp.dot(
        normed,
        both_halves(*[(m, None) for m in matrices], *[(None, m) for m in matrices]),
        preferred_element_type=F32,
    ).astype(BF16)
    out_matrix = jnp.concatenate([wo_ref[...], wo_ref[...]], axis=0)
    lane = lax.broadcasted_iota(jnp.int32, (min(per_line, QUERY_BLOCK), lanes), 1)
    place = lax.broadcasted_iota(jnp.int32, (owners, lanes), 0) % (pairs // own)

    def attend(entries, values):
        blended = blend(
            [(jnp.concatenate([low, high], axis=0), *keys) for low, high, keys in entries],
            values,
            scaling,
        )
        terms = [project_out(part, out_matrix) for part in blended]
        half = lane.shape[0]
        return [jnp.where(lane < channels, term[:half], term[half:]) for term in terms]

    def flipped_values():
        swapped = jnp.concatenate([normed[:, channels:], normed[:, :channels]], axis=1)
        every = jnp.concatenate(
            [
                part[v * per_line : (v + 1) * per_line]
                for v in range(local_v)
                for part in (normed, swapped)
            ],
            axis=0,
        )
        padded = jnp.concatenate([wv_ref[...], jnp.zeros_like(wv_ref[...])], axis=0)
        whole = turned(padded, every)
        return [whole[:, 2 * v * per_line : 2 * (v + 1) * per_line] for v in range(local_v)]

    entries = []
    for v in range(local_v):
        span = slice(v * per_line, (v + 1) * per_line)
        parts = [projected[span, i * width : (i + 1) * width] for i in range(4)]
        entries.append((*parts[::2], [jnp.concatenate(parts[1::2], axis=0)]))
    results = in_blocks(per_line, attend, entries, flipped_values, lines, mixed)
    for v, terms in enumerate(results):
        span = slice(v * per_line, (v + 1) * per_line)
        spread[v, pl.ds(SUBLANES, per_line), :] = tokens[span] + terms
        for step in range(window):
            piece = spread[v, pl.ds(SUBLANES - 1 + step, owners, stride=own), :]
            if step == 0:
                piece = jnp.where(place == 0, 0.0, piece)
            if step == window - 1:
                piece = jnp.where(place == pairs // own - 1, 0.0, piece)
            leaving[pl.ds(v * window + step, owners, stride=chunk), :] = piece
    o_ref[...] = leaving[...].astype(BF16).reshape(o_ref.shape)
    for copy in later:
        copy.wait()


def pair_weights(kernel):
    nothing = jnp.zeros_like(kernel[0, 0])
    parts = [[], [], [], []]
    for row in range(3):
        left, middle, right = kernel[row, 0], kernel[row, 1], kernel[row, 2]
        parts[0] += [middle, left]
        parts[1] += [right, middle]
        parts[2] += [nothing, right]
        parts[3] += [left, nothing]
    return jnp.concatenate([jnp.concatenate(part, axis=1) for part in parts], axis=0)


def correlate(images, weights, row):
    count, lanes = images[0].shape
    lane = lax.broadcasted_iota(jnp.int32, (count, lanes), 1)
    wide = [
        jnp.concatenate([image, jnp.where(lane < lanes // 2, after, before)], axis=1)
        for before, image, after in zip(images, images[1:], images[2:])
    ]
    terms = jnp.dot(jnp.concatenate(wide, axis=0), weights, preferred_element_type=F32)
    blank = jnp.zeros((row, lanes), F32)
    results = []
    for step in range(len(wide)):
        span = terms[step * count : (step + 1) * count]
        above = jnp.concatenate([blank, span[:-row, :lanes]], axis=0)
        below = jnp.concatenate([span[row:, 2 * lanes :], blank], axis=0)
        results.append(above + span[:, lanes : 2 * lanes] + below)
    return results


def columns_kernel(
    x_ref,
    wq_ref,
    wk_ref,
    wv_ref,
    wo_ref,
    first_ref,
    second_ref,
    o_ref,
    held,
    lines,
    mixed,
    *,
    local_v,
    views,
    places,
):
    sources, chunk, lanes = x_ref.shape
    channels, width = wq_ref.shape
    window = chunk // local_v
    own = window - 2
    per_line = sources * local_v
    row = views * local_v
    scaling = 1.0 / math.sqrt(width)
    rows = sources // views
    slots = [source % rows * views + source // rows for source in range(sources)]
    for source, slot in enumerate(slots):
        held[pl.ds(slot * chunk, chunk), :] = x_ref[source].astype(F32)
    tokens = jnp.concatenate(
        [held[pl.ds(step, per_line, stride=window), :] for step in range(window)], axis=0
    )
    normed = packed_norm(tokens, channels)
    matrices = [wq_ref[...], wk_ref[...]]
    projected = jnp.dot(
        normed,
        both_halves(*[(m, None) for m in matrices], *[(None, m) for m in matrices]),
        preferred_element_type=F32,
    ).astype(BF16)
    out_matrix = out_halves(wo_ref[...])

    def attend(entries, values):
        blended = blend(
            [
                line
                for low, high, keys in entries
                for line in ((low, keys[0]), (high, keys[1]))
            ],
            values,
            scaling,
        )
        return [
            project_out(jnp.concatenate(pair, axis=0), out_matrix)
            for pair in zip(blended[::2], blended[1::2])
        ]

    spans = [slice(step * per_line, (step + 1) * per_line) for step in range(window)]

    def flipped_values():
        whole = turned(both_halves((wv_ref[...], None), (None, wv_ref[...])), normed)
        return [
            whole[half * width : (half + 1) * width, span] for span in spans for half in range(2)
        ]

    entries = []
    for span in spans:
        parts = [projected[span, i * width : (i + 1) * width] for i in range(4)]
        entries.append((*parts[::2], parts[1::2]))
    results = in_blocks(per_line, attend, entries, flipped_values, lines, mixed)
    images = [(tokens[span] + terms).astype(BF16) for span, terms in zip(spans, results)]

    blank = jnp.zeros_like(images[0])
    hidden = [
        jnp.where(value >= 0, value, 0.1 * value)
        for value in correlate([blank, *images, blank], pair_weights(first_ref[...]), row)
    ]
    place = (lax.axis_index("view") * rows + lax.axis_index("line")) % places
    hidden[0] = jnp.where(place > 0, hidden[0], 0.0)
    hidden[-1] = jnp.where(place < places - 1, hidden[-1], 0.0)
    hidden = [value.astype(BF16) for value in hidden]
    for step, value in enumerate(correlate(hidden, pair_weights(second_ref[...]), row)):
        result = (images[step + 1].astype(F32) + value).astype(BF16)
        for source, slot in enumerate(slots):
            o_ref[source * own + step] = result[slot * local_v : (slot + 1) * local_v]


def local(light_field, query_weight, key_weight, value_weight, out_weight, conv_first, conv_second):
    span_rows, all_u, local_v, packed = light_field.shape
    channels, width = query_weight.shape[1:]
    lanes = 2 * channels
    lines, views = lax.axis_size("line"), lax.axis_size("view")
    devices = lines * views
    pairs = packed // lanes
    packed_lines = pairs * all_u
    own = packed_lines // devices
    if span_rows != 1 or packed_lines % devices or pairs % own:
        raise ValueError("unsupported split")
    window = own + 2
    places = pairs // own

    weights = (query_weight, key_weight, value_weight, out_weight.transpose(0, 2, 1))
    params = pltpu.CompilerParams(vmem_limit_bytes=VMEM_BYTES)

    def scratch(tokens):
        kept = tokens if tokens > QUERY_BLOCK else 16
        return [pltpu.VMEM((2, kept, width), BF16), pltpu.VMEM((kept, lanes), F32)]

    weights = (*weights, conv_first, conv_second)
    leaving, *later = pl.pallas_call(
        rows_kernel,
        out_shape=[
            jax.ShapeDtypeStruct((devices, local_v * window, lanes), BF16),
            *[jax.ShapeDtypeStruct((channels, width), BF16)] * 4,
            jax.ShapeDtypeStruct(conv_first.shape, BF16),
            jax.ShapeDtypeStruct(conv_second.shape, BF16),
        ],
        in_specs=[pl.BlockSpec(memory_space=pltpu.HBM)] * 7,
        scratch_shapes=[
            pltpu.VMEM((packed_lines * local_v, lanes), F32),
            pltpu.VMEM((local_v, packed_lines + 2 * SUBLANES, lanes), F32),
            pltpu.VMEM((devices * local_v * window, lanes), F32),
            *scratch(2 * packed_lines),
            pltpu.VMEM((all_u, local_v, packed), BF16),
            *[pltpu.VMEM((channels, width), BF16)] * 4,
            pltpu.SemaphoreType.DMA((11,)),
        ],
        compiler_params=params,
        name="rows",
    )(*(pltpu.with_memory_space_constraint(a, pltpu.HBM) for a in (light_field, *weights)))
    arrived = lax.all_to_all(leaving, AXES, split_axis=0, concat_axis=0, tiled=True)
    finished = pl.pallas_call(
        functools.partial(columns_kernel, local_v=local_v, views=views, places=places),
        out_shape=jax.ShapeDtypeStruct((packed_lines, local_v, lanes), BF16),
        scratch_shapes=[
            pltpu.VMEM((devices * local_v * window, lanes), F32),
            *scratch(devices * local_v),
        ],
        compiler_params=params,
        name="columns",
    )(arrived, *later)
    returned = lax.all_to_all(finished, AXES, split_axis=0, concat_axis=0, tiled=True)
    result = returned.reshape(all_u, pairs, local_v, lanes).transpose(0, 2, 1, 3)
    return result.reshape(light_field.shape)


def solution(mesh):
    placed = (P("line", None, "view", None), P(), P(), P(), P(), P(), P())
    return jax.shard_map(
        local, mesh=mesh, in_specs=placed, out_specs=P("line", None, "view", None), check_vma=False
    )
```

```python
import functools
import math

import jax
import jax.numpy as jnp
from jax import lax
from jax.experimental import pallas as pl
from jax.experimental.pallas import tpu as pltpu
from jax.sharding import PartitionSpec as P

AXES = ("view", "line")
QUERY_BLOCK = 256
F32 = jnp.float32
BF16 = jnp.bfloat16
SUBLANES = 8
VMEM_BYTES = 16 * 1024 * 1024


def block_ones(lanes, channels):
    rows = lax.broadcasted_iota(jnp.int32, (lanes, lanes), 0) // channels
    cols = lax.broadcasted_iota(jnp.int32, (lanes, lanes), 1) // channels
    return jnp.where(rows == cols, 1.0 / channels, 0.0).astype(F32)


def packed_norm(tokens, channels):
    ones = block_ones(tokens.shape[-1], channels)
    mean = jnp.dot(tokens.astype(BF16), ones.astype(BF16), preferred_element_type=F32)
    centre = tokens - mean
    square = centre * centre
    upper = square.astype(BF16)
    lower = (square - upper.astype(F32)).astype(BF16)
    spread = jnp.dot(
        jnp.concatenate([upper, lower], axis=1),
        jnp.concatenate([ones, ones], axis=0).astype(BF16),
        preferred_element_type=F32,
    )
    return (centre * lax.rsqrt(spread + 1e-05)).astype(BF16)


def both_halves(*parts):
    lower, upper = [], []
    for first, second in parts:
        lower.append(jnp.zeros_like(second) if first is None else first)
        upper.append(jnp.zeros_like(first) if second is None else second)
    return jnp.concatenate(
        [jnp.concatenate(lower, axis=1), jnp.concatenate(upper, axis=1)], axis=0
    )


def score(queries, keys, scaling):
    return (
        lax.dot_general(keys, queries, (((1,), (1,)), ((), ())), preferred_element_type=F32)
        * scaling
    )


def soften(scores):
    exponent = jnp.exp(scores - jnp.max(scores, axis=0, keepdims=True))
    return (exponent * (1.0 / jnp.sum(exponent, axis=0, keepdims=True))).astype(BF16)


def blend(lines, values, scaling):
    values = values()
    scores = [score(queries, keys, scaling) for queries, keys in lines]
    weights = [soften(part) for part in scores]
    return [
        jnp.dot(part, weight, preferred_element_type=F32).astype(BF16)
        for part, weight in zip(values, weights)
    ]


def in_blocks(count, attend, lines, values, pieces, mixed):
    if count <= QUERY_BLOCK:
        return attend(lines, values)
    values, results = values(), []
    for low, high, keys in lines:
        own_values = values[: len(keys)]
        values = values[len(keys) :]
        for index, part in enumerate([low, high]):
            pieces[index, :count] = part

        def block(index, carry, keys=keys, own_values=own_values):
            rows = pl.ds(pl.multiple_of(index * QUERY_BLOCK, QUERY_BLOCK), QUERY_BLOCK)
            line = (pieces[0, rows, :], pieces[1, rows, :], keys)
            (mixed[rows, :],) = attend([line], lambda: own_values)
            return carry

        lax.fori_loop(0, count // QUERY_BLOCK, block, 0)
        results.append(mixed[:count])
    return results


def out_halves(flipped):
    nothing = jnp.zeros_like(flipped)
    return jnp.concatenate(
        [
            jnp.concatenate([flipped, nothing], axis=1),
            jnp.concatenate([nothing, flipped], axis=1),
        ],
        axis=0,
    )


def project_out(blended, out_matrix):
    return lax.dot_general(
        blended, out_matrix, (((0,), (1,)), ((), ())), preferred_element_type=F32
    )


def turned(matrix, normed):
    return lax.dot_general(
        matrix, normed, (((0,), (1,)), ((), ())), preferred_element_type=F32
    ).astype(BF16)


def rows_kernel(
    x_hbm,
    wq_hbm,
    wk_hbm,
    wv_hbm,
    wo_hbm,
    first_hbm,
    second_hbm,
    o_ref,
    next_wq,
    next_wk,
    next_wv,
    next_wo,
    next_first,
    next_second,
    held,
    spread,
    leaving,
    lines,
    mixed,
    x_ref,
    wq_ref,
    wk_ref,
    wv_ref,
    wo_ref,
    arrivals,
):
    pulls = [
        (x_hbm, x_ref),
        (wq_hbm, wq_ref),
        (wk_hbm, wk_ref),
        (wv_hbm, wv_ref),
        (wo_hbm, wo_ref),
    ]
    copies = [
        pltpu.make_async_copy(source.at[0], target, arrivals.at[index])
        for index, (source, target) in enumerate(pulls)
    ]
    passed_on = [
        (wq_hbm.at[1], next_wq),
        (wk_hbm.at[1], next_wk),
        (wv_hbm.at[1], next_wv),
        (wo_hbm.at[1], next_wo),
        (first_hbm, next_first),
        (second_hbm, next_second),
    ]
    later = [
        pltpu.make_async_copy(source, target, arrivals.at[len(pulls) + index])
        for index, (source, target) in enumerate(passed_on)
    ]
    for copy in copies + later:
        copy.start()
    all_u, local_v, packed = x_ref.shape
    channels, width = wq_ref.shape
    lanes = 2 * channels
    pairs = packed // lanes
    per_line = pairs * all_u
    owners, chunk = o_ref.shape[:2]
    window = chunk // local_v
    own = window - 2
    scaling = 1.0 / math.sqrt(width)
    for copy in copies:
        copy.wait()
    for u in range(all_u):
        rows = x_ref[u].astype(F32)
        for pair in range(pairs):
            held[pl.ds((u * pairs + pair) * local_v, local_v), :] = rows[
                :, pair * lanes : (pair + 1) * lanes
            ]
    tokens = jnp.concatenate(
        [held[pl.ds(v, per_line, stride=local_v), :] for v in range(local_v)], axis=0
    )
    normed = packed_norm(tokens, channels)
    matrices = [wq_ref[...], wk_ref[...]]
    projected = jnp.dot(
        normed,
        both_halves(*[(m, None) for m in matrices], *[(None, m) for m in matrices]),
        preferred_element_type=F32,
    ).astype(BF16)
    out_matrix = jnp.concatenate([wo_ref[...], wo_ref[...]], axis=0)
    lane = lax.broadcasted_iota(jnp.int32, (min(per_line, QUERY_BLOCK), lanes), 1)
    place = lax.broadcasted_iota(jnp.int32, (owners, lanes), 0) % (pairs // own)

    def attend(entries, values):
        blended = blend(
            [(jnp.concatenate([low, high], axis=0), *keys) for low, high, keys in entries],
            values,
            scaling,
        )
        terms = [project_out(part, out_matrix) for part in blended]
        half = lane.shape[0]
        return [jnp.where(lane < channels, term[:half], term[half:]) for term in terms]

    def flipped_values():
        swapped = jnp.concatenate([normed[:, channels:], normed[:, :channels]], axis=1)
        every = jnp.concatenate(
            [
                part[v * per_line : (v + 1) * per_line]
                for v in range(local_v)
                for part in (normed, swapped)
            ],
            axis=0,
        )
        padded = jnp.concatenate([wv_ref[...], jnp.zeros_like(wv_ref[...])], axis=0)
        whole = turned(padded, every)
        return [whole[:, 2 * v * per_line : 2 * (v + 1) * per_line] for v in range(local_v)]

    entries = []
    for v in range(local_v):
        span = slice(v * per_line, (v + 1) * per_line)
        parts = [projected[span, i * width : (i + 1) * width] for i in range(4)]
        entries.append((*parts[::2], [jnp.concatenate(parts[1::2], axis=0)]))
    results = in_blocks(per_line, attend, entries, flipped_values, lines, mixed)
    for v, terms in enumerate(results):
        span = slice(v * per_line, (v + 1) * per_line)
        spread[v, pl.ds(SUBLANES, per_line), :] = tokens[span] + terms
        for step in range(window):
            piece = spread[v, pl.ds(SUBLANES - 1 + step, owners, stride=own), :]
            if step == 0:
                piece = jnp.where(place == 0, 0.0, piece)
            if step == window - 1:
                piece = jnp.where(place == pairs // own - 1, 0.0, piece)
            leaving[pl.ds(v * window + step, owners, stride=chunk), :] = piece
    o_ref[...] = leaving[...].astype(BF16).reshape(o_ref.shape)
    for copy in later:
        copy.wait()


def pair_weights(kernel):
    nothing = jnp.zeros_like(kernel[0, 0])
    parts = [[], [], [], []]
    for row in range(3):
        left, middle, right = kernel[row, 0], kernel[row, 1], kernel[row, 2]
        parts[0] += [middle, left]
        parts[1] += [right, middle]
        parts[2] += [nothing, right]
        parts[3] += [left, nothing]
    return jnp.concatenate([jnp.concatenate(part, axis=1) for part in parts], axis=0)


def correlate(images, weights, row):
    count, lanes = images[0].shape
    lane = lax.broadcasted_iota(jnp.int32, (count, lanes), 1)
    wide = [
        jnp.concatenate([image, jnp.where(lane < lanes // 2, after, before)], axis=1)
        for before, image, after in zip(images, images[1:], images[2:])
    ]
    terms = jnp.dot(jnp.concatenate(wide, axis=0), weights, preferred_element_type=F32)
    blank = jnp.zeros((row, lanes), F32)
    results = []
    for step in range(len(wide)):
        span = terms[step * count : (step + 1) * count]
        above = jnp.concatenate([blank, span[:-row, :lanes]], axis=0)
        below = jnp.concatenate([span[row:, 2 * lanes :], blank], axis=0)
        results.append(above + span[:, lanes : 2 * lanes] + below)
    return results


def columns_kernel(
    x_ref,
    wq_ref,
    wk_ref,
    wv_ref,
    wo_ref,
    first_ref,
    second_ref,
    o_ref,
    held,
    lines,
    mixed,
    *,
    local_v,
    views,
    places,
):
    sources, chunk, lanes = x_ref.shape
    channels, width = wq_ref.shape
    window = chunk // local_v
    own = window - 2
    per_line = sources * local_v
    row = views * local_v
    scaling = 1.0 / math.sqrt(width)
    rows = sources // views
    slots = [source % rows * views + source // rows for source in range(sources)]
    for source, slot in enumerate(slots):
        held[pl.ds(slot * chunk, chunk), :] = x_ref[source].astype(F32)
    tokens = jnp.concatenate(
        [held[pl.ds(step, per_line, stride=window), :] for step in range(window)], axis=0
    )
    normed = packed_norm(tokens, channels)
    matrices = [wq_ref[...], wk_ref[...]]
    projected = jnp.dot(
        normed,
        both_halves(*[(m, None) for m in matrices], *[(None, m) for m in matrices]),
        preferred_element_type=F32,
    ).astype(BF16)
    out_matrix = out_halves(wo_ref[...])

    def attend(entries, values):
        blended = blend(
            [
                line
                for low, high, keys in entries
                for line in ((low, keys[0]), (high, keys[1]))
            ],
            values,
            scaling,
        )
        return [
            project_out(jnp.concatenate(pair, axis=0), out_matrix)
            for pair in zip(blended[::2], blended[1::2])
        ]

    spans = [slice(step * per_line, (step + 1) * per_line) for step in range(window)]

    def flipped_values():
        whole = turned(both_halves((wv_ref[...], None), (None, wv_ref[...])), normed)
        return [
            whole[half * width : (half + 1) * width, span] for span in spans for half in range(2)
        ]

    entries = []
    for span in spans:
        parts = [projected[span, i * width : (i + 1) * width] for i in range(4)]
        entries.append((*parts[::2], parts[1::2]))
    results = in_blocks(per_line, attend, entries, flipped_values, lines, mixed)
    images = [(tokens[span] + terms).astype(BF16) for span, terms in zip(spans, results)]

    blank = jnp.zeros_like(images[0])
    hidden = [
        jnp.where(value >= 0, value, 0.1 * value)
        for value in correlate([blank, *images, blank], pair_weights(first_ref[...]), row)
    ]
    place = (lax.axis_index("view") * rows + lax.axis_index("line")) % places
    hidden[0] = jnp.where(place > 0, hidden[0], 0.0)
    hidden[-1] = jnp.where(place < places - 1, hidden[-1], 0.0)
    hidden = [value.astype(BF16) for value in hidden]
    for step, value in enumerate(correlate(hidden, pair_weights(second_ref[...]), row)):
        result = (images[step + 1].astype(F32) + value).astype(BF16)
        for source, slot in enumerate(slots):
            o_ref[source * own + step] = result[slot * local_v : (slot + 1) * local_v]


def local(light_field, query_weight, key_weight, value_weight, out_weight, conv_first, conv_second):
    span_rows, all_u, local_v, packed = light_field.shape
    channels, width = query_weight.shape[1:]
    lanes = 2 * channels
    lines, views = lax.axis_size("line"), lax.axis_size("view")
    devices = lines * views
    pairs = packed // lanes
    packed_lines = pairs * all_u
    own = packed_lines // devices
    if span_rows != 1 or packed_lines % devices or pairs % own:
        raise ValueError("unsupported split")
    window = own + 2
    places = pairs // own

    weights = (query_weight, key_weight, value_weight, out_weight.transpose(0, 2, 1))
    params = pltpu.CompilerParams(vmem_limit_bytes=VMEM_BYTES)

    def scratch(tokens):
        kept = tokens if tokens > QUERY_BLOCK else 16
        return [pltpu.VMEM((2, kept, width), BF16), pltpu.VMEM((kept, lanes), F32)]

    weights = (*weights, conv_first, conv_second)
    leaving, *later = pl.pallas_call(
        rows_kernel,
        out_shape=[
            jax.ShapeDtypeStruct((devices, local_v * window, lanes), BF16),
            *[jax.ShapeDtypeStruct((channels, width), BF16)] * 4,
            jax.ShapeDtypeStruct(conv_first.shape, BF16),
            jax.ShapeDtypeStruct(conv_second.shape, BF16),
        ],
        in_specs=[pl.BlockSpec(memory_space=pltpu.HBM)] * 7,
        scratch_shapes=[
            pltpu.VMEM((packed_lines * local_v, lanes), F32),
            pltpu.VMEM((local_v, packed_lines + 2 * SUBLANES, lanes), F32),
            pltpu.VMEM((devices * local_v * window, lanes), F32),
            *scratch(2 * packed_lines),
            pltpu.VMEM((all_u, local_v, packed), BF16),
            *[pltpu.VMEM((channels, width), BF16)] * 4,
            pltpu.SemaphoreType.DMA((11,)),
        ],
        compiler_params=params,
        name="rows",
    )(*(pltpu.with_memory_space_constraint(a, pltpu.HBM) for a in (light_field, *weights)))
    arrived = lax.all_to_all(leaving, AXES, split_axis=0, concat_axis=0, tiled=True)
    finished = pl.pallas_call(
        functools.partial(columns_kernel, local_v=local_v, views=views, places=places),
        out_shape=jax.ShapeDtypeStruct((packed_lines, local_v, lanes), BF16),
        scratch_shapes=[
            pltpu.VMEM((devices * local_v * window, lanes), F32),
            *scratch(devices * local_v),
        ],
        compiler_params=params,
        name="columns",
    )(arrived, *later)
    returned = lax.all_to_all(finished, AXES, split_axis=0, concat_axis=0, tiled=True)
    result = returned.reshape(all_u, pairs, local_v, lanes).transpose(0, 2, 1, 3)
    return result.reshape(light_field.shape)


def solution(mesh):
    placed = (P("line", None, "view", None), P(), P(), P(), P(), P(), P())
    return jax.shard_map(
        local, mesh=mesh, in_specs=placed, out_specs=P("line", None, "view", None), check_vma=False
    )
```

```python
import functools
import math

import jax
import jax.numpy as jnp
from jax import lax
from jax.experimental import pallas as pl
from jax.experimental.pallas import tpu as pltpu
from jax.sharding import PartitionSpec as P

AXES = ("view", "line")
QUERY_BLOCK = 256
F32 = jnp.float32
BF16 = jnp.bfloat16
SUBLANES = 8
PARTS = 1
VMEM_BYTES = 16 * 1024 * 1024


def block_ones(lanes, channels):
    rows = lax.broadcasted_iota(jnp.int32, (lanes, lanes), 0) // channels
    cols = lax.broadcasted_iota(jnp.int32, (lanes, lanes), 1) // channels
    return jnp.where(rows == cols, 1.0 / channels, 0.0).astype(F32)


def packed_norm(tokens, channels):
    ones = block_ones(tokens.shape[-1], channels)
    mean = jnp.dot(tokens.astype(BF16), ones.astype(BF16), preferred_element_type=F32)
    centre = tokens - mean
    square = centre * centre
    upper = square.astype(BF16)
    lower = (square - upper.astype(F32)).astype(BF16)
    spread = jnp.dot(
        jnp.concatenate([upper, lower], axis=1),
        jnp.concatenate([ones, ones], axis=0).astype(BF16),
        preferred_element_type=F32,
    )
    return (centre * lax.rsqrt(spread + 1e-05)).astype(BF16)


def both_halves(*parts):
    lower, upper = [], []
    for first, second in parts:
        lower.append(jnp.zeros_like(second) if first is None else first)
        upper.append(jnp.zeros_like(first) if second is None else second)
    return jnp.concatenate(
        [jnp.concatenate(lower, axis=1), jnp.concatenate(upper, axis=1)], axis=0
    )


def score(queries, keys, scaling):
    return (
        lax.dot_general(keys, queries, (((1,), (1,)), ((), ())), preferred_element_type=F32)
        * scaling
    )


def soften(scores):
    exponent = jnp.exp(scores - jnp.max(scores, axis=0, keepdims=True))
    return (exponent * (1.0 / jnp.sum(exponent, axis=0, keepdims=True))).astype(BF16)


def blend(lines, values, scaling):
    values = values()
    scores = [score(queries, keys, scaling) for queries, keys in lines]
    weights = [soften(part) for part in scores]
    return [
        jnp.dot(part, weight, preferred_element_type=F32).astype(BF16)
        for part, weight in zip(values, weights)
    ]


def in_blocks(count, attend, lines, values, pieces, mixed):
    if count <= QUERY_BLOCK:
        return attend(lines, values)
    values, results = values(), []
    for low, high, keys in lines:
        own_values = values[: len(keys)]
        values = values[len(keys) :]
        for index, part in enumerate([low, high]):
            pieces[index, :count] = part

        def block(index, carry, keys=keys, own_values=own_values):
            rows = pl.ds(pl.multiple_of(index * QUERY_BLOCK, QUERY_BLOCK), QUERY_BLOCK)
            line = (pieces[0, rows, :], pieces[1, rows, :], keys)
            (mixed[rows, :],) = attend([line], lambda: own_values)
            return carry

        lax.fori_loop(0, count // QUERY_BLOCK, block, 0)
        results.append(mixed[:count])
    return results


def out_halves(flipped):
    nothing = jnp.zeros_like(flipped)
    return jnp.concatenate(
        [
            jnp.concatenate([flipped, nothing], axis=1),
            jnp.concatenate([nothing, flipped], axis=1),
        ],
        axis=0,
    )


def project_out(blended, out_matrix):
    return lax.dot_general(
        blended, out_matrix, (((0,), (1,)), ((), ())), preferred_element_type=F32
    )


def turned(matrix, normed):
    return lax.dot_general(
        matrix, normed, (((0,), (1,)), ((), ())), preferred_element_type=F32
    ).astype(BF16)


def rows_kernel(
    x_hbm,
    wq_hbm,
    wk_hbm,
    wv_hbm,
    wo_hbm,
    first_hbm,
    second_hbm,
    o_ref,
    next_wq,
    next_wk,
    next_wv,
    next_wo,
    next_first,
    next_second,
    held,
    spread,
    leaving,
    lines,
    mixed,
    x_ref,
    wq_ref,
    wk_ref,
    wv_ref,
    wo_ref,
    arrivals,
):
    pulls = [
        (x_hbm, x_ref),
        (wq_hbm, wq_ref),
        (wk_hbm, wk_ref),
        (wv_hbm, wv_ref),
        (wo_hbm, wo_ref),
    ]
    copies = [
        pltpu.make_async_copy(source.at[0], target, arrivals.at[index])
        for index, (source, target) in enumerate(pulls)
    ]
    passed_on = [
        (wq_hbm.at[1], next_wq),
        (wk_hbm.at[1], next_wk),
        (wv_hbm.at[1], next_wv),
        (wo_hbm.at[1], next_wo),
        (first_hbm, next_first),
        (second_hbm, next_second),
    ]
    later = [
        pltpu.make_async_copy(source, target, arrivals.at[len(pulls) + index])
        for index, (source, target) in enumerate(passed_on)
    ]
    for copy in copies + later:
        copy.start()
    all_u, local_v, packed = x_ref.shape
    channels, width = wq_ref.shape
    lanes = 2 * channels
    pairs = packed // lanes
    per_line = pairs * all_u
    owners, chunk = o_ref.shape[:2]
    window = chunk // local_v
    own = window - 2
    scaling = 1.0 / math.sqrt(width)
    for copy in copies:
        copy.wait()
    for u in range(all_u):
        rows = x_ref[u].astype(F32)
        for pair in range(pairs):
            held[pl.ds((u * pairs + pair) * local_v, local_v), :] = rows[
                :, pair * lanes : (pair + 1) * lanes
            ]
    tokens = jnp.concatenate(
        [held[pl.ds(v, per_line, stride=local_v), :] for v in range(local_v)], axis=0
    )
    normed = packed_norm(tokens, channels)
    matrices = [wq_ref[...], wk_ref[...]]
    projected = jnp.dot(
        normed,
        both_halves(*[(m, None) for m in matrices], *[(None, m) for m in matrices]),
        preferred_element_type=F32,
    ).astype(BF16)
    out_matrix = jnp.concatenate([wo_ref[...], wo_ref[...]], axis=0)
    lane = lax.broadcasted_iota(jnp.int32, (min(per_line, QUERY_BLOCK), lanes), 1)
    place = lax.broadcasted_iota(jnp.int32, (owners, lanes), 0) % (pairs // own)

    def attend(entries, values):
        blended = blend(
            [(jnp.concatenate([low, high], axis=0), *keys) for low, high, keys in entries],
            values,
            scaling,
        )
        terms = [project_out(part, out_matrix) for part in blended]
        half = lane.shape[0]
        return [jnp.where(lane < channels, term[:half], term[half:]) for term in terms]

    def flipped_values():
        swapped = jnp.concatenate([normed[:, channels:], normed[:, :channels]], axis=1)
        every = jnp.concatenate(
            [
                part[v * per_line : (v + 1) * per_line]
                for v in range(local_v)
                for part in (normed, swapped)
            ],
            axis=0,
        )
        padded = jnp.concatenate([wv_ref[...], jnp.zeros_like(wv_ref[...])], axis=0)
        whole = turned(padded, every)
        return [whole[:, 2 * v * per_line : 2 * (v + 1) * per_line] for v in range(local_v)]

    entries = []
    for v in range(local_v):
        span = slice(v * per_line, (v + 1) * per_line)
        parts = [projected[span, i * width : (i + 1) * width] for i in range(4)]
        entries.append((*parts[::2], [jnp.concatenate(parts[1::2], axis=0)]))
    results = in_blocks(per_line, attend, entries, flipped_values, lines, mixed)
    for v, terms in enumerate(results):
        span = slice(v * per_line, (v + 1) * per_line)
        spread[v, pl.ds(SUBLANES, per_line), :] = tokens[span] + terms
        for step in range(window):
            piece = spread[v, pl.ds(SUBLANES - 1 + step, owners, stride=own), :]
            if step == 0:
                piece = jnp.where(place == 0, 0.0, piece)
            if step == window - 1:
                piece = jnp.where(place == pairs // own - 1, 0.0, piece)
            leaving[pl.ds(v * window + step, owners, stride=chunk), :] = piece
    o_ref[...] = leaving[...].astype(BF16).reshape(o_ref.shape)
    for copy in later:
        copy.wait()


def pair_weights(kernel):
    nothing = jnp.zeros_like(kernel[0, 0])
    parts = [[], [], [], []]
    for row in range(3):
        left, middle, right = kernel[row, 0], kernel[row, 1], kernel[row, 2]
        parts[0] += [middle, left]
        parts[1] += [right, middle]
        parts[2] += [nothing, right]
        parts[3] += [left, nothing]
    return jnp.concatenate([jnp.concatenate(part, axis=1) for part in parts], axis=0)


def correlate(images, weights, row):
    count, lanes = images[0].shape
    lane = lax.broadcasted_iota(jnp.int32, (count, lanes), 1)
    wide = [
        jnp.concatenate([image, jnp.where(lane < lanes // 2, after, before)], axis=1)
        for before, image, after in zip(images, images[1:], images[2:])
    ]
    terms = jnp.dot(jnp.concatenate(wide, axis=0), weights, preferred_element_type=F32)
    blank = jnp.zeros((row, lanes), F32)
    results = []
    for step in range(len(wide)):
        span = terms[step * count : (step + 1) * count]
        above = jnp.concatenate([blank, span[:-row, :lanes]], axis=0)
        below = jnp.concatenate([span[row:, 2 * lanes :], blank], axis=0)
        results.append(above + span[:, lanes : 2 * lanes] + below)
    return results


def columns_kernel(
    x_ref,
    wq_ref,
    wk_ref,
    wv_ref,
    wo_ref,
    first_ref,
    second_ref,
    o_ref,
    held,
    lines,
    mixed,
    *,
    local_v,
    views,
    places,
):
    sources, chunk, lanes = x_ref.shape
    channels, width = wq_ref.shape
    window = chunk // local_v
    own = window - 2
    per_line = sources * local_v
    row = views * local_v
    scaling = 1.0 / math.sqrt(width)
    rows = sources // views
    slots = [source % rows * views + source // rows for source in range(sources)]
    for source, slot in enumerate(slots):
        held[pl.ds(slot * chunk, chunk), :] = x_ref[source].astype(F32)
    tokens = jnp.concatenate(
        [held[pl.ds(step, per_line, stride=window), :] for step in range(window)], axis=0
    )
    normed = packed_norm(tokens, channels)
    matrices = [wq_ref[...], wk_ref[...]]
    projected = jnp.dot(
        normed,
        both_halves(*[(m, None) for m in matrices], *[(None, m) for m in matrices]),
        preferred_element_type=F32,
    ).astype(BF16)
    out_matrix = out_halves(wo_ref[...])

    def attend(entries, values):
        blended = blend(
            [
                line
                for low, high, keys in entries
                for line in ((low, keys[0]), (high, keys[1]))
            ],
            values,
            scaling,
        )
        return [
            project_out(jnp.concatenate(pair, axis=0), out_matrix)
            for pair in zip(blended[::2], blended[1::2])
        ]

    spans = [slice(step * per_line, (step + 1) * per_line) for step in range(window)]

    def flipped_values():
        whole = turned(both_halves((wv_ref[...], None), (None, wv_ref[...])), normed)
        return [
            whole[half * width : (half + 1) * width, span] for span in spans for half in range(2)
        ]

    entries = []
    for span in spans:
        parts = [projected[span, i * width : (i + 1) * width] for i in range(4)]
        entries.append((*parts[::2], parts[1::2]))
    results = in_blocks(per_line, attend, entries, flipped_values, lines, mixed)
    images = [(tokens[span] + terms).astype(BF16) for span, terms in zip(spans, results)]

    blank = jnp.zeros_like(images[0])
    hidden = [
        jnp.where(value >= 0, value, 0.1 * value)
        for value in correlate([blank, *images, blank], pair_weights(first_ref[...]), row)
    ]
    place = (lax.axis_index("view") * rows + lax.axis_index("line")) % places
    hidden[0] = jnp.where(place > 0, hidden[0], 0.0)
    hidden[-1] = jnp.where(place < places - 1, hidden[-1], 0.0)
    hidden = [value.astype(BF16) for value in hidden]
    for step, value in enumerate(correlate(hidden, pair_weights(second_ref[...]), row)):
        result = (images[step + 1].astype(F32) + value).astype(BF16)
        for source, slot in enumerate(slots):
            o_ref[source * own + step] = result[slot * local_v : (slot + 1) * local_v]


def place_kernel(x_ref, o_hbm, departures):
    share = x_ref.shape[0] // PARTS
    copies = [
        pltpu.make_async_copy(
            x_ref.at[pl.ds(part * share, share)],
            o_hbm.at[pl.ds(part * share, share)],
            departures.at[part],
        )
        for part in range(PARTS)
    ]
    for copy in copies:
        copy.start()
    for copy in copies:
        copy.wait()


def local(light_field, query_weight, key_weight, value_weight, out_weight, conv_first, conv_second):
    span_rows, all_u, local_v, packed = light_field.shape
    channels, width = query_weight.shape[1:]
    lanes = 2 * channels
    lines, views = lax.axis_size("line"), lax.axis_size("view")
    devices = lines * views
    pairs = packed // lanes
    packed_lines = pairs * all_u
    own = packed_lines // devices
    if span_rows != 1 or packed_lines % devices or pairs % own:
        raise ValueError("unsupported split")
    window = own + 2
    places = pairs // own

    weights = (query_weight, key_weight, value_weight, out_weight.transpose(0, 2, 1))
    params = pltpu.CompilerParams(vmem_limit_bytes=VMEM_BYTES)

    def scratch(tokens):
        kept = tokens if tokens > QUERY_BLOCK else 16
        return [pltpu.VMEM((2, kept, width), BF16), pltpu.VMEM((kept, lanes), F32)]

    weights = (*weights, conv_first, conv_second)
    leaving, *later = pl.pallas_call(
        rows_kernel,
        out_shape=[
            jax.ShapeDtypeStruct((devices, local_v * window, lanes), BF16),
            *[jax.ShapeDtypeStruct((channels, width), BF16)] * 4,
            jax.ShapeDtypeStruct(conv_first.shape, BF16),
            jax.ShapeDtypeStruct(conv_second.shape, BF16),
        ],
        in_specs=[pl.BlockSpec(memory_space=pltpu.HBM)] * 7,
        scratch_shapes=[
            pltpu.VMEM((packed_lines * local_v, lanes), F32),
            pltpu.VMEM((local_v, packed_lines + 2 * SUBLANES, lanes), F32),
            pltpu.VMEM((devices * local_v * window, lanes), F32),
            *scratch(2 * packed_lines),
            pltpu.VMEM((all_u, local_v, packed), BF16),
            *[pltpu.VMEM((channels, width), BF16)] * 4,
            pltpu.SemaphoreType.DMA((11,)),
        ],
        compiler_params=params,
        name="rows",
    )(*(pltpu.with_memory_space_constraint(a, pltpu.HBM) for a in (light_field, *weights)))
    arrived = lax.all_to_all(leaving, AXES, split_axis=0, concat_axis=0, tiled=True)
    finished = pl.pallas_call(
        functools.partial(columns_kernel, local_v=local_v, views=views, places=places),
        out_shape=jax.ShapeDtypeStruct((packed_lines, local_v, lanes), BF16),
        scratch_shapes=[
            pltpu.VMEM((devices * local_v * window, lanes), F32),
            *scratch(devices * local_v),
        ],
        compiler_params=params,
        name="columns",
    )(arrived, *later)
    returned = lax.all_to_all(finished, AXES, split_axis=0, concat_axis=0, tiled=True)
    returned = pl.pallas_call(
        place_kernel,
        out_shape=jax.ShapeDtypeStruct(returned.shape, BF16),
        in_specs=[pl.BlockSpec(memory_space=pltpu.VMEM)],
        out_specs=pl.BlockSpec(memory_space=pltpu.HBM),
        scratch_shapes=[pltpu.SemaphoreType.DMA((PARTS,))],
        compiler_params=params,
        name="place",
    )(returned)
    result = returned.reshape(all_u, pairs, local_v, lanes).transpose(0, 2, 1, 3)
    return result.reshape(light_field.shape)


def solution(mesh):
    placed = (P("line", None, "view", None), P(), P(), P(), P(), P(), P())
    return jax.shard_map(
        local, mesh=mesh, in_specs=placed, out_specs=P("line", None, "view", None), check_vma=False
    )
```
